32 devices in a mesh: vtx: 8 (over z, x), src: 4 (over y, core).
Axes of the slice: x: 2, y: 2, z: 4, core: 2. Of those that a mesh axis runs over, the one named last changes fastest.
Arguments:
- heat: float32 [64, 64, 8192], P(None, ('vtx', 'src')), may hold values from -12 to 12
- cotan: float32 [4, 64, 8192], P(None, 'vtx'), may hold values from 0.2 to 2
- source_index: int32 [64], replicated, may hold values from 0 to 524287
Outputs:
- normalised: float32 [64, 64, 8192], P('src', 'vtx')
- col_norm: float32 [64], P('src')
The draws below stay inside these ranges and needn't reach their ends.
Inputs may be any that keep to these rules, and one draw needn't show every extreme that they name: `source_index`: row-major vertex indices, sources may share a vertex.
All inputs are finite; a program needn't handle non-finite values.
Results may differ from the reference program's by a relative error of at most 0.0003.
Values sent between devices are 32-bit elements; how exact they have to be, the bound alone decides.
No kernel may reach another device: no remote copies, remote signals or barrier semaphores. Data moves between devices by JAX's collectives and lax.ppermute only.
A program may use at most 64 MiB of HBM per device.

```python
import math
import jax
import jax.numpy as jnp
from jax import lax

SOURCES = 64
GX = 8192
GY = 64


def draw_heat(key, part):
    rows = jnp.arange(GY, dtype=jnp.float32) / max(GY - 1, 1)
    base_key = jax.random.fold_in(key, 11)
    factor_key = jax.random.fold_in(key, 23)
    row_factor = jax.random.uniform(factor_key, (SOURCES, GY), jnp.float32, 0.3, 1.0)
    base = jnp.clip(jax.random.normal(base_key, (SOURCES, GY, GX), jnp.float32), -4.0, 4.0)
    scale = 1.0 + 2.0 * rows
    return base * (scale[None, :] * row_factor)[:, :, None]


def plant(entries, stream_key, smallest, top_value):
    longest = entries.shape.index(max(entries.shape))
    spots = []
    for shift in (0, 1):
        where = [jax.random.randint(jax.random.fold_in(stream_key, axis), (), 0, length) for axis, length in enumerate(entries.shape)]
        where[longest] = (where[longest] + shift) % entries.shape[longest]
        spots.append(tuple(where))
    return entries.at[spots[0]].set(smallest).at[spots[1]].set(top_value)


def shard_levels(rng, shape, cuts, least, largest):
    loudness, own = 1.0, jax.random.fold_in(rng, 6)
    for axis_at, blocks in cuts:
        heights = jnp.exp(jax.random.uniform(jax.random.fold_in(own, axis_at), (blocks,), jnp.float32, least / len(cuts), largest / len(cuts)))
        loudness = loudness * jnp.repeat(heights, shape[axis_at] // blocks).reshape([-1 if axis == axis_at else 1 for axis in range(len(shape))])
    return loudness


def setup_inputs(seed: int = 0) -> dict:
    streams_of = jax.random.split(jax.random.key(seed), 4)
    return {
        "heat": draw_heat(jax.random.fold_in(streams_of[3], 71), 0),
        "cotan": jnp.clip(jnp.exp(math.log(2.0) - 2.3025851 * jax.random.uniform(streams_of[1], (4, GY, GX), jnp.float32) ** shard_levels(streams_of[1], (4, GY, GX), ((1, 8),), -0.2, 0.2)), 0.2, 2.0),
        "source_index": plant(jax.random.randint(streams_of[2], (SOURCES,), 0, GY * GX), jax.random.fold_in(streams_of[2], 1), 0, (GY * GX) - 1).astype(jnp.int32),
    }


def from_right(values):
    return jnp.concatenate([values[..., 1:], jnp.zeros_like(values[..., :1])], axis=-1)

def from_left(values):
    return jnp.concatenate([jnp.zeros_like(values[..., :1]), values[..., :-1]], axis=-1)

def masked_cotan(cotan, row_start, total_rows):
    shape = cotan.shape[1:]
    rows = row_start + lax.broadcasted_iota(jnp.int32, shape, 0)
    cols = lax.broadcasted_iota(jnp.int32, shape, 1)
    inside_col = cols < shape[1] - 1
    inside_row = rows < total_rows - 1
    mass = cotan[0]
    east = jnp.where(inside_col, cotan[1], 0.0)
    north = jnp.where(inside_row, cotan[2], 0.0)
    diag = jnp.where(inside_col & inside_row, cotan[3], 0.0)
    return (mass, east, north, diag)

def stencil_defect(padded, mass, east, north_ext, diag_ext, row_start, sources, amplitude):
    center = padded[:, 1:-1, :]
    above = padded[:, 2:, :]
    below = padded[:, :-2, :]
    north = north_ext[1:]
    south_weight = north_ext[:-1]
    diag = diag_ext[1:]
    southwest_weight = from_left(diag_ext[:-1])
    west_weight = from_left(east)
    result = mass * center + east * (center - from_right(center))
    result = result + west_weight * (center - from_left(center))
    result = result + north * (center - above) + south_weight * (center - below)
    result = result + diag * (center - from_right(above)) + southwest_weight * (center - from_left(below))
    count_rows, width = (center.shape[1], center.shape[2])
    row_ids = row_start + lax.broadcasted_iota(jnp.int32, (count_rows, width), 0)
    col_ids = lax.broadcasted_iota(jnp.int32, (count_rows, width), 1)
    flat = row_ids * width + col_ids
    delta = (flat[None, :, :] == sources.astype(jnp.int32)[:, None, None]).astype(jnp.float32)
    return result - amplitude * delta

def reference(heat, cotan, source_index):
    total_rows, width = (heat.shape[1], heat.shape[2])
    amplitude = math.sqrt(total_rows * width) / 8.0
    mass, east, north, diag = masked_cotan(cotan, 0, total_rows)
    north_ext = jnp.concatenate([jnp.zeros((1, width), jnp.float32), north], axis=0)
    diag_ext = jnp.concatenate([jnp.zeros((1, width), jnp.float32), diag], axis=0)

    def single(inputs):
        field, source = inputs
        padded = jnp.pad(field[None], ((0, 0), (1, 1), (0, 0)))
        result = stencil_defect(padded, mass, east, north_ext, diag_ext, 0, source[None], amplitude)[0]
        return (result, jnp.sum(result * result))
    defect, squares = lax.map(single, (heat, source_index))
    norms = jnp.sqrt(squares / (total_rows * width) + 1e-06)
    return (defect / norms[:, None, None], norms)
```

```python
import functools
import math

import jax
import jax.numpy as jnp
from jax import lax
from jax.experimental import pallas as pl
from jax.experimental.pallas import tpu as pltpu
from jax.sharding import PartitionSpec as P

LANES = 128
SUB = 8
PAD = 8


def weights_kernel(meta, place, cotan, lower, out):
    rows_dev, cb, total_rows = meta
    lane = lax.broadcasted_iota(jnp.int32, (SUB, LANES), 1)
    index = lax.broadcasted_iota(jnp.int32, (SUB, LANES), 0) * LANES + lane
    last_lane = lane == LANES - 1

    def column_step(q, _):
        at = pl.ds(pl.multiple_of(q * SUB, SUB), SUB)
        inside_left = index + q * SUB * LANES > 0
        inside_right = index + q * SUB * LANES < cb * LANES - 1

        def row_of(array, row, back=0):
            return cotan[pl.ds((array * cb + q * SUB - back) * rows_dev + row, SUB, stride=rows_dev), :]

        def from_left(value, before):
            moved = pltpu.roll(jnp.where(last_lane, before, value), 1, 1)
            return jnp.where(inside_left, moved, 0.0)

        south = lower[pl.ds(pl.multiple_of(q * SUB, SUB), SUB), :]
        southwest = from_left(
            lower[pl.ds(pl.multiple_of(cb + q * SUB, SUB), SUB), :], lower[pl.ds(cb - 1 + q * SUB, SUB), :]
        )
        for row in range(rows_dev):
            inside_row = jnp.full((SUB, LANES), place[1] + row, jnp.int32) < total_rows - 1
            east = row_of(1, row)
            west = from_left(east, row_of(1, row, 1))
            east = jnp.where(inside_right, east, 0.0)
            north = jnp.where(inside_row, row_of(2, row), 0.0)
            raw = row_of(3, row)
            diag = jnp.where(inside_right & inside_row, raw, 0.0)
            centre = row_of(0, row) + east + west + north + south + diag + southwest
            for w, value in enumerate((centre, east, west, north, south, diag, southwest)):
                out[w, row, at, :] = value
            south, southwest = north, from_left(raw, row_of(3, row, 1))
        return 0

    lax.fori_loop(0, cb // SUB, column_step, 0)


def defect_kernel(meta, lo, n, group, amplitude, *refs):
    pieces, rows_dev, cb, senders, own_rows = meta
    n_in = len(pieces)
    place, sources, weights = refs[:3]
    ins = refs[3 : 3 + n_in]
    prev = refs[3 + n_in] if lo else None
    out, sums = refs[-4:-2]
    grid, sem = refs[-2:]
    me = place[0]
    copies = []
    for at, (ref, (kind, k, first, count, skip)) in enumerate(zip(ins, pieces, strict=True)):
        t = me ^ k
        low = t < senders // 2
        if kind == "below":
            row = 0
        elif kind == "above":
            row = rows_dev + 1
        elif kind == "outer":
            row = 1 + t * own_rows + jnp.where(low, 0, own_rows - 1)
        else:
            row = 1 + t * own_rows + kind + jnp.where(low, 1, 0)
        copy = pltpu.make_async_copy(
            ref.at[pl.ds(skip * cb, count * cb), :],
            grid.at[row, pl.ds(PAD + (first - lo) * cb, count * cb), :],
            sem.at[at],
        )
        copy.start()
        copies.append(copy)
    zero = jnp.zeros((SUB, LANES), jnp.float32)
    for row in range(rows_dev + 2):
        grid[row, pl.ds(0, PAD), :] = zero
        grid[row, pl.ds(PAD + n * cb, PAD), :] = zero
    if lo:
        sums[...] = prev[...]
    else:
        sums[...] = jnp.zeros(sums.shape, jnp.float32)
    for copy in copies:
        copy.wait()
    lane = lax.broadcasted_iota(jnp.int32, (SUB, LANES), 1)
    index = lax.broadcasted_iota(jnp.int32, (SUB, LANES), 0) * LANES + lane
    first_lane, last_lane = lane == 0, lane == LANES - 1
    width = cb * LANES
    start = place[1] * width

    def source_step(i, _):
        source = sources[me * group + lo + i] - start

        def column_step(q, total):
            base = pl.multiple_of(PAD + i * cb + q * SUB, SUB)
            at = pl.ds(pl.multiple_of(q * SUB, SUB), SUB)
            here, right, left = [], [], []
            for row in range(rows_dev + 2):
                value = grid[row, pl.ds(base, SUB), :]
                here.append(value)
                after = grid[row, pl.ds(base + 1, SUB), :] if row else None
                right.append(pltpu.roll(jnp.where(first_lane, after, value), LANES - 1, 1) if row else None)
                if row <= rows_dev:
                    before = grid[row, pl.ds(base - 1, SUB), :]
                    left.append(pltpu.roll(jnp.where(last_lane, before, value), 1, 1))
            for row in range(rows_dev):
                c = [weights[w, row, at, :] for w in range(7)]
                value = c[0] * here[row + 1] - c[1] * right[row + 1] - c[2] * left[row + 1]
                value = value - c[3] * here[row + 2] - c[4] * here[row]
                value = value - c[5] * right[row + 2] - c[6] * left[row]
                spot = source - row * width - q * SUB * LANES
                value = value - jnp.where(index == spot, amplitude, 0.0)
                out[pl.ds((i * cb + q * SUB) * rows_dev + row, SUB, stride=rows_dev), :] = value
                total = total + value * value
            return total

        total = lax.fori_loop(0, cb // SUB, column_step, zero)
        sums[pl.ds(lo + i, 1), :] = jnp.sum(total, axis=0, keepdims=True)
        return 0

    lax.fori_loop(0, n, source_step, 0)


def scale_kernel(chunks, size, *refs):
    total, parts, out, norms, buf, in_sem, out_sem = refs[0], refs[1:-5], *refs[-5:]
    group, per = total.shape[0], out.shape[0] // total.shape[0]
    reads, writes = [], []
    for part, (lo, n) in zip(parts, chunks, strict=True):
        for i in range(n):
            spot = pl.ds((lo + i) * per, per)
            copy = pltpu.make_async_copy(part.at[pl.ds(i * per, per), :], buf.at[spot, :], in_sem.at[lo + i])
            copy.start()
            reads.append(copy)
            writes.append(pltpu.make_async_copy(buf.at[spot, :], out.at[spot, :], out_sem.at[lo + i]))
    sums = jnp.sum(total[...], axis=1, keepdims=True)
    norm = jnp.sqrt(sums / size + 1e-06)
    lane = lax.broadcasted_iota(jnp.int32, (group, LANES), 1)
    sub = lax.broadcasted_iota(jnp.int32, (group, LANES), 0)
    spread = jnp.where(lane == sub, jnp.broadcast_to(norm, (group, LANES)), 0.0)
    norms[...] = jnp.sum(spread, axis=0, keepdims=True)[:, :group]
    inverse = jnp.broadcast_to(1.0 / norm, (group, LANES))
    for i in range(group):
        reads[i].wait()
        factor = jnp.broadcast_to(inverse[i : i + 1], (SUB, LANES))

        def step(j, _, i=i, factor=factor):
            for u in range(8):
                at = pl.ds(pl.multiple_of(i * per + (j * 8 + u) * SUB, SUB), SUB)
                buf[at, :] = buf[at, :] * factor
            return 0

        lax.fori_loop(0, per // (SUB * 8), step, 0)
        writes[i].start()
    for write in writes:
        write.wait()


def on_device(heat, cotan, source_index):
    peers, senders = lax.axis_size("vtx"), lax.axis_size("src")
    all_sources, own_rows, width = heat.shape
    rows_dev = cotan.shape[1]
    total_rows = rows_dev * peers
    group = all_sources // senders
    cb = width // LANES
    amplitude = math.sqrt(total_rows * width) / 8.0
    me, block = lax.axis_index("src"), lax.axis_index("vtx")
    block_start = block * rows_dev
    low = me < senders // 2
    outer_row = (0, own_rows - 1)

    def send(k, row, first, count):
        to = me ^ k
        piece = lax.dynamic_slice(heat, (to * group + first, 0, 0), (count, own_rows, width))
        piece = jnp.where(low, piece[:, row[0]], piece[:, row[1]]).reshape(count * cb, LANES)
        if k:
            piece = lax.ppermute(piece, "src", [(i, i ^ k) for i in range(senders)])
        return piece

    order = [k for k in range(1, senders) if k >= 2] + [1, 0]
    halves = [(0, group // 2), (group // 2, group - group // 2)]
    chunks = [(0, group - group // 4), (group - group // 4, group // 4)]
    outer = [{k: send(k, outer_row, *half) for k in order} for half in halves]
    inner = [[{k: send(k, (1 + j, j), *chunk) for k in order} for j in range(own_rows - 1)] for chunk in chunks]
    up = [(i, i + 1) for i in range(peers - 1)]
    down = [(j, i) for i, j in up]
    anywhere = pl.BlockSpec(memory_space=pl.ANY)
    vmem = pl.BlockSpec(memory_space=pltpu.VMEM)
    smem = pl.BlockSpec(memory_space=pltpu.SMEM)
    place = jnp.stack([me, block_start])
    per = cb * rows_dev
    lower = lax.ppermute(cotan[2:4, rows_dev - 1].reshape(2 * cb, LANES), "vtx", up)
    tiles = cotan.reshape(4, rows_dev, cb, LANES).transpose(0, 2, 1, 3).reshape(4 * per, LANES)
    weights = pl.pallas_call(
        functools.partial(weights_kernel, (rows_dev, cb, total_rows)),
        out_shape=jax.ShapeDtypeStruct((7, rows_dev, cb, LANES), jnp.float32),
        in_specs=[smem, vmem, vmem],
        out_specs=vmem,
        cost_estimate=pl.CostEstimate(flops=20 * per * LANES, bytes_accessed=44 * per * LANES, transcendentals=0),
        name="weights",
    )(place, tiles, lower)
    below, above = [], []
    for got in outer:
        first = lax.select_n(me, *[got[k] for k in range(senders)])
        last = lax.select_n(me, *[got[k] for k in reversed(range(senders))])
        above.append(lax.ppermute(first, "vtx", down))
        below.append(lax.ppermute(last, "vtx", up))

    parts, sums = [], None
    for c, (lo, n) in enumerate(chunks):
        pieces, ins = [], []

        def take(kind, k, first, count, array):
            begin, end = max(first, lo), min(first + count, lo + n)
            if begin < end:
                pieces.append((kind, k, begin, end - begin, begin - first))
                ins.append(array)

        for half, got, b, a in zip(halves, outer, below, above, strict=True):
            for k in range(senders):
                take("outer", k, *half, got[k])
            take("below", 0, *half, b)
            take("above", 0, *half, a)
        for j in range(own_rows - 1):
            for k in range(senders):
                take(j, k, lo, n, inner[c][j][k])
        meta = (tuple(pieces), rows_dev, cb, senders, own_rows)
        part, sums = pl.pallas_call(
            functools.partial(defect_kernel, meta, lo, n, group, amplitude),
            out_shape=(
                jax.ShapeDtypeStruct((n * per, LANES), jnp.float32),
                jax.ShapeDtypeStruct((group, LANES), jnp.float32),
            ),
            in_specs=[smem, smem, vmem] + [anywhere] * len(ins) + ([vmem] if lo else []),
            out_specs=(vmem, vmem),
            scratch_shapes=[
                pltpu.VMEM((rows_dev + 2, n * cb + 2 * PAD, LANES), jnp.float32),
                pltpu.SemaphoreType.DMA((len(ins),)),
            ],
            cost_estimate=pl.CostEstimate(flops=20 * n * per * LANES, bytes_accessed=8 * n * per * LANES, transcendentals=0),
            name="defect",
        )(place, source_index, weights, *ins, *([sums] if lo else []))
        parts.append(part)
    step = 1
    while step < peers:
        sums = sums + lax.ppermute(sums, "vtx", [(i, i ^ step) for i in range(peers)])
        step *= 2
    out, norms = pl.pallas_call(
        functools.partial(scale_kernel, chunks, float(total_rows * width)),
        out_shape=(
            jax.ShapeDtypeStruct((group * per, LANES), jnp.float32),
            jax.ShapeDtypeStruct((1, group), jnp.float32),
        ),
        in_specs=[vmem] + [anywhere] * len(parts),
        out_specs=(anywhere, vmem),
        scratch_shapes=[
            pltpu.VMEM((group * per, LANES), jnp.float32),
            pltpu.SemaphoreType.DMA((group,)),
            pltpu.SemaphoreType.DMA((group,)),
        ],
        cost_estimate=pl.CostEstimate(flops=group * per * LANES, bytes_accessed=8 * group * per * LANES, transcendentals=0),
        name="scale",
    )(sums, *parts)
    out = out.reshape(group, cb, rows_dev, LANES).transpose(0, 2, 1, 3).reshape(group, rows_dev, width)
    return out, norms.reshape(group)


def solution(mesh):
    return jax.shard_map(
        on_device,
        mesh=mesh,
        in_specs=(P(None, ("vtx", "src"), None), P(None, "vtx", None), P()),
        out_specs=(P("src", "vtx", None), P("src")),
        check_vma=False,
    )
```

```python
import functools
import math

import jax
import jax.numpy as jnp
from jax import lax
from jax.experimental import pallas as pl
from jax.experimental.pallas import tpu as pltpu
from jax.sharding import PartitionSpec as P

LANES = 128
SUB = 8
PAD = 8
TAIL = 16


def pack_kernel(meta, heat, *refs):
    blocks, group, cb, own_rows, senders = meta
    n_out = max(out for *_, targets in blocks for out, *_ in targets) + 1
    outs = refs[:n_out]
    wide, in_sem = refs[n_out:]
    me = lax.axis_index("src")
    low = me < senders // 2
    reads, at = [], 0
    for b, (k, lo, n, _) in enumerate(blocks):
        size = n * cb * own_rows
        copy = pltpu.make_async_copy(
            heat.at[pl.ds(((me ^ k) * group + lo) * cb * own_rows, size), :], wide.at[pl.ds(at, size), :], in_sem.at[b]
        )
        copy.start()
        reads.append((copy, at))
        at += size
    for (copy, at), (k, lo, n, targets) in zip(reads, blocks, strict=True):
        copy.wait()
        for out, rows, skip, first, count in targets:
            start = at + skip * cb * own_rows + jnp.where(low, rows[0], rows[1])

            def step(i, _, start=start, ref=outs[out], first=first):
                for u in range(cb // SUB):
                    to = pl.multiple_of((first + i) * cb + u * SUB, SUB)
                    ref[pl.ds(to, SUB), :] = wide[pl.ds(start + (i * cb + u * SUB) * own_rows, SUB, stride=own_rows), :]
                return 0

            lax.fori_loop(0, count, step, 0)


def pack(heat, wanted, blocks, group, cb, own_rows, senders, name):
    plan = []
    for k, lo, n in blocks:
        targets = []
        for out, (wk, rows, first, count) in enumerate(wanted):
            begin, end = max(lo, first), min(lo + n, first + count)
            if wk == k and begin < end:
                targets.append((out, rows, begin - lo, begin - first, end - begin))
        plan.append((k, lo, n, tuple(targets)))
    reads = sum(n for _, n in ((k, n) for k, _, n in blocks)) * cb * own_rows
    writes = sum(count for *_, count in wanted) * cb
    vmem = pl.BlockSpec(memory_space=pltpu.VMEM)
    return pl.pallas_call(
        functools.partial(pack_kernel, (tuple(plan), group, cb, own_rows, senders)),
        out_shape=tuple(jax.ShapeDtypeStruct((count * cb, LANES), jnp.float32) for *_, count in wanted),
        in_specs=[pl.BlockSpec(memory_space=pltpu.HBM)],
        out_specs=tuple(vmem for _ in wanted),
        scratch_shapes=[
            pltpu.VMEM((reads, LANES), jnp.float32),
            pltpu.SemaphoreType.DMA((len(blocks),)),
        ],
        compiler_params=pltpu.CompilerParams(vmem_limit_bytes=16 << 20),
        cost_estimate=pl.CostEstimate(flops=writes * LANES, bytes_accessed=4 * (reads + writes) * LANES, transcendentals=0),
        name=name,
    )(heat)


def weights_kernel(meta, cotan, lower, out):
    rows_dev, cb, total_rows = meta
    block_start = lax.axis_index("vtx") * rows_dev
    lane = lax.broadcasted_iota(jnp.int32, (SUB, LANES), 1)
    index = lax.broadcasted_iota(jnp.int32, (SUB, LANES), 0) * LANES + lane
    last_lane = lane == LANES - 1

    def column_step(q, _):
        at = pl.ds(pl.multiple_of(q * SUB, SUB), SUB)
        inside_left = index + q * SUB * LANES > 0
        inside_right = index + q * SUB * LANES < cb * LANES - 1

        def row_of(array, row, back=0):
            return cotan[pl.ds((array * cb + q * SUB - back) * rows_dev + row, SUB, stride=rows_dev), :]

        def from_left(value, before):
            moved = pltpu.roll(jnp.where(last_lane, before, value), 1, 1)
            return jnp.where(inside_left, moved, 0.0)

        south = lower[pl.ds(pl.multiple_of(q * SUB, SUB), SUB), :]
        southwest = from_left(
            lower[pl.ds(pl.multiple_of(cb + q * SUB, SUB), SUB), :], lower[pl.ds(cb - 1 + q * SUB, SUB), :]
        )
        for row in range(rows_dev):
            inside_row = jnp.full((SUB, LANES), block_start + row, jnp.int32) < total_rows - 1
            east = row_of(1, row)
            west = from_left(east, row_of(1, row, 1))
            east = jnp.where(inside_right, east, 0.0)
            north = jnp.where(inside_row, row_of(2, row), 0.0)
            raw = row_of(3, row)
            diag = jnp.where(inside_right & inside_row, raw, 0.0)
            centre = row_of(0, row) + east + west + north + south + diag + southwest
            for w, value in enumerate((centre, east, west, north, south, diag, southwest)):
                out[w, row, at, :] = value
            south, southwest = north, from_left(raw, row_of(3, row, 1))
        return 0

    lax.fori_loop(0, cb // SUB, column_step, 0)


def defect_kernel(meta, lo, n, group, amplitude, *refs):
    pieces, rows_dev, cb, senders, own_rows = meta
    n_in = len(pieces)
    sources, weights = refs[:2]
    ins = refs[2 : 2 + n_in]
    prev = refs[2 + n_in] if lo else None
    out, sums, grid = refs[-3:]
    me = lax.axis_index("src")
    for ref, (kind, k, first, count, skip) in zip(ins, pieces, strict=True):
        t = me ^ k
        low = t < senders // 2
        if kind == "below":
            row = 0
        elif kind == "above":
            row = rows_dev + 1
        elif kind == "outer":
            row = 1 + t * own_rows + jnp.where(low, 0, own_rows - 1)
        else:
            row = 1 + t * own_rows + kind + jnp.where(low, 1, 0)

        def move(i, _, ref=ref, row=row, first=first, skip=skip):
            for u in range(cb // SUB):
                to = pl.multiple_of(PAD + (first - lo + i) * cb + u * SUB, SUB)
                grid[row, pl.ds(to, SUB), :] = ref[pl.ds(pl.multiple_of((skip + i) * cb + u * SUB, SUB), SUB), :]
            return 0

        lax.fori_loop(0, count, move, 0)
    zero = jnp.zeros((SUB, LANES), jnp.float32)
    for row in range(rows_dev + 2):
        grid[row, pl.ds(0, PAD), :] = zero
        grid[row, pl.ds(PAD + n * cb, PAD), :] = zero
    if lo:
        sums[...] = prev[...]
    else:
        sums[...] = jnp.zeros(sums.shape, jnp.float32)
    lane = lax.broadcasted_iota(jnp.int32, (SUB, LANES), 1)
    index = lax.broadcasted_iota(jnp.int32, (SUB, LANES), 0) * LANES + lane
    first_lane, last_lane = lane == 0, lane == LANES - 1
    width = cb * LANES
    start = lax.axis_index("vtx") * rows_dev * width

    def source_step(i, _):
        source = sources[me * group + lo + i] - start

        def column_step(q, total):
            base = pl.multiple_of(PAD + i * cb + q * SUB, SUB)
            at = pl.ds(pl.multiple_of(q * SUB, SUB), SUB)
            here, right, left = [], [], []
            for row in range(rows_dev + 2):
                value = grid[row, pl.ds(base, SUB), :]
                here.append(value)
                after = grid[row, pl.ds(base + 1, SUB), :] if row else None
                right.append(pltpu.roll(jnp.where(first_lane, after, value), LANES - 1, 1) if row else None)
                if row <= rows_dev:
                    before = grid[row, pl.ds(base - 1, SUB), :]
                    left.append(pltpu.roll(jnp.where(last_lane, before, value), 1, 1))
            for row in range(rows_dev):
                c = [weights[w, row, at, :] for w in range(7)]
                value = c[0] * here[row + 1] - c[1] * right[row + 1] - c[2] * left[row + 1]
                value = value - c[3] * here[row + 2] - c[4] * here[row]
                value = value - c[5] * right[row + 2] - c[6] * left[row]
                spot = source - row * width - q * SUB * LANES
                value = value - jnp.where(index == spot, amplitude, 0.0)
                out[pl.ds((i * cb + q * SUB) * rows_dev + row, SUB, stride=rows_dev), :] = value
                total = total + value * value
            return total

        total = lax.fori_loop(0, cb // SUB, column_step, zero)
        sums[pl.ds(lo + i, 1), :] = jnp.sum(total, axis=0, keepdims=True)
        return 0

    lax.fori_loop(0, n, source_step, 0)


def scale_kernel(chunks, size, *refs):
    mine, other, parts, out, norms, buf, out_sem = refs[0], refs[1], refs[2:-4], *refs[-4:]
    group, per = mine.shape[0], out.shape[0] // mine.shape[0]
    sums = jnp.sum(mine[...] + other[...], axis=1, keepdims=True)
    norm = jnp.sqrt(sums / size + 1e-06)
    lane = lax.broadcasted_iota(jnp.int32, (group, LANES), 1)
    sub = lax.broadcasted_iota(jnp.int32, (group, LANES), 0)
    spread = jnp.where(lane == sub, jnp.broadcast_to(norm, (group, LANES)), 0.0)
    norms[...] = jnp.sum(spread, axis=0, keepdims=True)[:, :group]
    inverse = jnp.broadcast_to(1.0 / norm, (group, LANES))
    writes = []
    for i in range(group):
        part, (lo, n) = [(p, c) for p, c in zip(parts, chunks, strict=True) if c[0] <= i < sum(c)][0]
        factor = jnp.broadcast_to(inverse[i : i + 1], (SUB, LANES))

        def step(j, _, i=i, lo=lo, part=part, factor=factor):
            for u in range(8):
                at = (j * 8 + u) * SUB
                to = pl.ds(pl.multiple_of(i * per + at, SUB), SUB)
                buf[to, :] = part[pl.ds(pl.multiple_of((i - lo) * per + at, SUB), SUB), :] * factor
            return 0

        lax.fori_loop(0, per // (SUB * 8), step, 0)
        spot = pl.ds(i * per, per)
        writes.append(pltpu.make_async_copy(buf.at[spot, :], out.at[spot, :], out_sem.at[i]))
        writes[-1].start()
    for write in writes:
        write.wait()


def on_device(heat, cotan, source_index):
    peers, senders = lax.axis_size("vtx"), lax.axis_size("src")
    all_sources, own_rows, width = heat.shape
    rows_dev = cotan.shape[1]
    total_rows = rows_dev * peers
    group = all_sources // senders
    cb = width // LANES
    amplitude = math.sqrt(total_rows * width) / 8.0
    me = lax.axis_index("src")
    view = heat.reshape(all_sources, own_rows, cb, LANES).transpose(0, 2, 1, 3).reshape(-1, LANES)
    outer_rows = (0, own_rows - 1)
    order = [k for k in range(1, senders) if k >= 2] + [1]
    halves = [(0, group // 2), (group // 2, group - group // 2)]
    chunks = [(0, group - group // 4), (group - group // 4, group // 4)]
    common = (group, cb, own_rows, senders)

    def send(k, piece):
        return lax.ppermute(piece, "src", [(i, i ^ k) for i in range(senders)]) if k else piece

    first_wanted = [(k, outer_rows, *halves[0]) for k in order[:-1]]
    wanted = [(k, outer_rows, *halves[1]) for k in order]
    wanted += [(k, outer_rows, *halves[0]) for k in (1, 0)] + [(0, outer_rows, *halves[1])]
    wanted += [(k, (1 + j, j), *chunk) for chunk in chunks for j in range(own_rows - 1) for k in order + [0]]
    packed = pack(view, first_wanted, [(k, *halves[0]) for k in order[:-1]], *common, "pack_first")
    table = dict(zip(first_wanted, packed, strict=True))
    packed = pack(view, wanted, [(k, *half) for half in reversed(halves) for k in order + [0]], *common, "pack_rest")
    table.update(zip(wanted, packed, strict=True))
    table = {key: send(key[0], piece) for key, piece in table.items()}
    outer = [{k: table[k, outer_rows, *half] for k in range(senders)} for half in halves]
    inner = [
        [{k: table[k, (1 + j, j), *chunk] for k in range(senders)} for j in range(own_rows - 1)] for chunk in chunks
    ]
    up = [(i, i + 1) for i in range(peers - 1)]
    down = [(j, i) for i, j in up]
    vmem = pl.BlockSpec(memory_space=pltpu.VMEM)
    smem = pl.BlockSpec(memory_space=pltpu.SMEM)
    per = cb * rows_dev
    lower = lax.ppermute(cotan[2:4, rows_dev - 1].reshape(2 * cb, LANES), "vtx", up)
    tiles = cotan.reshape(4, rows_dev, cb, LANES).transpose(0, 2, 1, 3).reshape(4 * per, LANES)
    weights = pl.pallas_call(
        functools.partial(weights_kernel, (rows_dev, cb, total_rows)),
        out_shape=jax.ShapeDtypeStruct((7, rows_dev, cb + PAD, LANES), jnp.float32),
        in_specs=[vmem, vmem],
        out_specs=vmem,
        compiler_params=pltpu.CompilerParams(vmem_limit_bytes=8 << 20),
        cost_estimate=pl.CostEstimate(flops=20 * per * LANES, bytes_accessed=44 * per * LANES, transcendentals=0),
        name="weights",
    )(tiles, lower)
    below, above = [], []
    for got in outer:
        first = lax.select_n(me, *[got[k] for k in range(senders)])
        last = lax.select_n(me, *[got[k] for k in reversed(range(senders))])
        above.append(lax.ppermute(first, "vtx", down))
        below.append(lax.ppermute(last, "vtx", up))

    parts, sums = [], None
    for c, (lo, n) in enumerate(chunks):
        pieces, ins = [], []

        def take(kind, k, first, count, array):
            begin, end = max(first, lo), min(first + count, lo + n)
            if begin < end:
                pieces.append((kind, k, begin, end - begin, begin - first))
                ins.append(array)

        for half, got, b, a in zip(halves, outer, below, above, strict=True):
            for k in range(senders):
                take("outer", k, *half, got[k])
            take("below", 0, *half, b)
            take("above", 0, *half, a)
        for j in range(own_rows - 1):
            for k in range(senders):
                take(j, k, lo, n, inner[c][j][k])
        meta = (tuple(pieces), rows_dev, cb, senders, own_rows)
        part, sums = pl.pallas_call(
            functools.partial(defect_kernel, meta, lo, n, group, amplitude),
            out_shape=(
                jax.ShapeDtypeStruct((n * per, LANES), jnp.float32),
                jax.ShapeDtypeStruct((group, LANES), jnp.float32),
            ),
            in_specs=[smem, vmem] + [vmem] * len(ins) + ([vmem] if lo else []),
            out_specs=(vmem, vmem),
            scratch_shapes=[
                pltpu.VMEM((rows_dev + 2, n * cb + PAD + TAIL, LANES), jnp.float32),
            ],
            cost_estimate=pl.CostEstimate(flops=20 * n * per * LANES, bytes_accessed=8 * n * per * LANES, transcendentals=0),
            compiler_params=pltpu.CompilerParams(vmem_limit_bytes=24 << 20),
            name="defect",
        )(source_index, weights, *ins, *([sums] if lo else []))
        parts.append(part)
    step, other = 1, None
    while step < peers:
        sums = sums if other is None else sums + other
        other = lax.ppermute(sums, "vtx", [(i, i ^ step) for i in range(peers)])
        step *= 2
    out, norms = pl.pallas_call(
        functools.partial(scale_kernel, chunks, float(total_rows * width)),
        out_shape=(
            jax.ShapeDtypeStruct((group * per, LANES), jnp.float32),
            jax.ShapeDtypeStruct((1, group), jnp.float32),
        ),
        in_specs=[vmem, vmem] + [vmem] * len(parts),
        out_specs=(pl.BlockSpec(memory_space=pltpu.HBM), vmem),
        scratch_shapes=[
            pltpu.VMEM((group * per, LANES), jnp.float32),
            pltpu.SemaphoreType.DMA((group,)),
        ],
        cost_estimate=pl.CostEstimate(flops=group * per * LANES, bytes_accessed=8 * group * per * LANES, transcendentals=0),
        compiler_params=pltpu.CompilerParams(vmem_limit_bytes=12 << 20),
        name="scale",
    )(sums, other, *parts)
    out = out.reshape(group, cb, rows_dev, LANES).transpose(0, 2, 1, 3).reshape(group, rows_dev, width)
    return out, norms.reshape(group)


def solution(mesh):
    return jax.shard_map(
        on_device,
        mesh=mesh,
        in_specs=(P(None, ("vtx", "src"), None), P(None, "vtx", None), P()),
        out_specs=(P("src", "vtx", None), P("src")),
        check_vma=False,
    )
```

```python
import functools
import math

import jax
import jax.numpy as jnp
from jax import lax
from jax.experimental import pallas as pl
from jax.experimental.pallas import tpu as pltpu
from jax.sharding import PartitionSpec as P


LANES = 128
SUB = 8
PAD = 8
TAIL = 16


def pack_kernel(meta, heat, *refs):
    blocks, group, cb, own_rows, senders = meta
    n_out = max(out for *_, targets in blocks for out, *_ in targets) + 1
    outs = refs[:n_out]
    wide, in_sem = refs[n_out:]
    me = lax.axis_index("src")
    low = me < senders // 2
    reads, at = [], 0
    for b, (k, lo, n, _) in enumerate(blocks):
        size = n * cb * own_rows
        copy = pltpu.make_async_copy(
            heat.at[pl.ds(((me ^ k) * group + lo) * cb * own_rows, size), :], wide.at[pl.ds(at, size), :], in_sem.at[b]
        )
        copy.start()
        reads.append((copy, at))
        at += size
    for (copy, at), (k, lo, n, targets) in zip(reads, blocks, strict=True):
        copy.wait()
        for out, rows, skip, first, count in targets:
            start = at + skip * cb * own_rows + jnp.where(low, rows[0], rows[1])

            def step(i, _, start=start, ref=outs[out], first=first):
                for u in range(cb // SUB):
                    to = pl.multiple_of((first + i) * cb + u * SUB, SUB)
                    ref[pl.ds(to, SUB), :] = wide[pl.ds(start + (i * cb + u * SUB) * own_rows, SUB, stride=own_rows), :]
                return 0

            lax.fori_loop(0, count, step, 0)


def pack(heat, wanted, blocks, group, cb, own_rows, senders, limit):
    plan = []
    for k, lo, n in blocks:
        targets = []
        for out, (wk, rows, first, count) in enumerate(wanted):
            begin, end = max(lo, first), min(lo + n, first + count)
            if wk == k and begin < end:
                targets.append((out, rows, begin - lo, begin - first, end - begin))
        plan.append((k, lo, n, tuple(targets)))
    reads = sum(n for _, n in ((k, n) for k, _, n in blocks)) * cb * own_rows
    writes = sum(count for *_, count in wanted) * cb
    vmem = pl.BlockSpec(memory_space=pltpu.VMEM)
    return pl.pallas_call(
        functools.partial(pack_kernel, (tuple(plan), group, cb, own_rows, senders)),
        out_shape=tuple(jax.ShapeDtypeStruct((count * cb, LANES), jnp.float32) for *_, count in wanted),
        in_specs=[pl.BlockSpec(memory_space=pltpu.HBM)],
        out_specs=tuple(vmem for _ in wanted),
        scratch_shapes=[
            pltpu.VMEM((reads, LANES), jnp.float32),
            pltpu.SemaphoreType.DMA((len(blocks),)),
        ],
        compiler_params=pltpu.CompilerParams(vmem_limit_bytes=limit << 20),
        cost_estimate=pl.CostEstimate(flops=writes * LANES, bytes_accessed=4 * (reads + writes) * LANES, transcendentals=0),
    )(heat)


def weights_kernel(meta, cotan, lower, out):
    rows_dev, cb, total_rows = meta
    block_start = lax.axis_index("vtx") * rows_dev
    lane = lax.broadcasted_iota(jnp.int32, (SUB, LANES), 1)
    index = lax.broadcasted_iota(jnp.int32, (SUB, LANES), 0) * LANES + lane
    last_lane = lane == LANES - 1

    def column_step(q, _):
        at = pl.ds(pl.multiple_of(q * SUB, SUB), SUB)
        inside_left = index + q * SUB * LANES > 0
        inside_right = index + q * SUB * LANES < cb * LANES - 1

        def row_of(array, row, back=0):
            return cotan[pl.ds((array * cb + q * SUB - back) * rows_dev + row, SUB, stride=rows_dev), :]

        def from_left(value, before):
            moved = pltpu.roll(jnp.where(last_lane, before, value), 1, 1)
            return jnp.where(inside_left, moved, 0.0)

        south = lower[pl.ds(pl.multiple_of(q * SUB, SUB), SUB), :]
        southwest = from_left(
            lower[pl.ds(pl.multiple_of(cb + q * SUB, SUB), SUB), :], lower[pl.ds(cb - 1 + q * SUB, SUB), :]
        )
        for row in range(rows_dev):
            inside_row = jnp.full((SUB, LANES), block_start + row, jnp.int32) < total_rows - 1
            east = row_of(1, row)
            west = from_left(east, row_of(1, row, 1))
            east = jnp.where(inside_right, east, 0.0)
            north = jnp.where(inside_row, row_of(2, row), 0.0)
            raw = row_of(3, row)
            diag = jnp.where(inside_right & inside_row, raw, 0.0)
            centre = row_of(0, row) + east + west + north + south + diag + southwest
            for w, value in enumerate((centre, east, west, north, south, diag, southwest)):
                out[w, row, at, :] = value
            south, southwest = north, from_left(raw, row_of(3, row, 1))
        return 0

    lax.fori_loop(0, cb // SUB, column_step, 0)


def defect_kernel(meta, lo, n, group, amplitude, *refs):
    pieces, rows_dev, cb, senders, own_rows = meta
    n_in = len(pieces)
    sources, weights = refs[:2]
    ins = refs[2 : 2 + n_in]
    prev = refs[2 + n_in] if lo else None
    out, sums, grid = refs[-3:]
    me = lax.axis_index("src")
    for ref, (kind, k, first, count, skip) in zip(ins, pieces, strict=True):
        t = me ^ k
        low = t < senders // 2
        if kind == "below":
            row = 0
        elif kind == "above":
            row = rows_dev + 1
        elif kind == "outer":
            row = 1 + t * own_rows + jnp.where(low, 0, own_rows - 1)
        else:
            row = 1 + t * own_rows + kind + jnp.where(low, 1, 0)

        def move(i, _, ref=ref, row=row, first=first, skip=skip):
            for u in range(cb // SUB):
                to = pl.multiple_of(PAD + (first - lo + i) * cb + u * SUB, SUB)
                grid[row, pl.ds(to, SUB), :] = ref[pl.ds(pl.multiple_of((skip + i) * cb + u * SUB, SUB), SUB), :]
            return 0

        lax.fori_loop(0, count, move, 0)
    zero = jnp.zeros((SUB, LANES), jnp.float32)
    for row in range(rows_dev + 2):
        grid[row, pl.ds(0, PAD), :] = zero
        grid[row, pl.ds(PAD + n * cb, PAD), :] = zero
    if lo:
        sums[...] = prev[...]
    else:
        sums[...] = jnp.zeros(sums.shape, jnp.float32)
    lane = lax.broadcasted_iota(jnp.int32, (SUB, LANES), 1)
    index = lax.broadcasted_iota(jnp.int32, (SUB, LANES), 0) * LANES + lane
    first_lane, last_lane = lane == 0, lane == LANES - 1
    width = cb * LANES
    start = lax.axis_index("vtx") * rows_dev * width

    def source_step(i, _):
        source = sources[me * group + lo + i] - start

        def column_step(q, total):
            base = pl.multiple_of(PAD + i * cb + q * SUB, SUB)
            at = pl.ds(pl.multiple_of(q * SUB, SUB), SUB)
            here, right, left = [], [], []
            for row in range(rows_dev + 2):
                value = grid[row, pl.ds(base, SUB), :]
                here.append(value)
                after = grid[row, pl.ds(base + 1, SUB), :] if row else None
                right.append(pltpu.roll(jnp.where(first_lane, after, value), LANES - 1, 1) if row else None)
                if row <= rows_dev:
                    before = grid[row, pl.ds(base - 1, SUB), :]
                    left.append(pltpu.roll(jnp.where(last_lane, before, value), 1, 1))
            for row in range(rows_dev):
                c = [weights[w, row, at, :] for w in range(7)]
                value = c[0] * here[row + 1] - c[1] * right[row + 1] - c[2] * left[row + 1]
                value = value - c[3] * here[row + 2] - c[4] * here[row]
                value = value - c[5] * right[row + 2] - c[6] * left[row]
                spot = source - row * width - q * SUB * LANES
                value = value - jnp.where(index == spot, amplitude, 0.0)
                out[pl.ds((i * cb + q * SUB) * rows_dev + row, SUB, stride=rows_dev), :] = value
                total = total + value * value
            return total

        total = lax.fori_loop(0, cb // SUB, column_step, zero, unroll=math.gcd(cb // SUB, 8))
        sums[pl.ds(lo + i, 1), :] = jnp.sum(total, axis=0, keepdims=True)
        return 0

    lax.fori_loop(0, n, source_step, 0)


def scale_kernel(chunks, size, *refs):
    mine, other, parts, out, norms, buf, out_sem = refs[0], refs[1], refs[2:-4], *refs[-4:]
    group, per = mine.shape[0], out.shape[0] // mine.shape[0]
    sums = jnp.sum(mine[...] + other[...], axis=1, keepdims=True)
    norm = jnp.sqrt(sums / size + 1e-06)
    lane = lax.broadcasted_iota(jnp.int32, (group, LANES), 1)
    sub = lax.broadcasted_iota(jnp.int32, (group, LANES), 0)
    spread = jnp.where(lane == sub, jnp.broadcast_to(norm, (group, LANES)), 0.0)
    norms[...] = jnp.sum(spread, axis=0, keepdims=True)[:, :group]
    inverse = jnp.broadcast_to(1.0 / norm, (group, LANES))
    writes = []
    for i in range(group):
        part, (lo, n) = [(p, c) for p, c in zip(parts, chunks, strict=True) if c[0] <= i < sum(c)][0]
        factor = jnp.broadcast_to(inverse[i : i + 1], (SUB, LANES))

        def step(j, _, i=i, lo=lo, part=part, factor=factor):
            for u in range(8):
                at = (j * 8 + u) * SUB
                to = pl.ds(pl.multiple_of(i * per + at, SUB), SUB)
                buf[to, :] = part[pl.ds(pl.multiple_of((i - lo) * per + at, SUB), SUB), :] * factor
            return 0

        lax.fori_loop(0, per // (SUB * 8), step, 0)
        spot = pl.ds(i * per, per)
        writes.append(pltpu.make_async_copy(buf.at[spot, :], out.at[spot, :], out_sem.at[i]))
        writes[-1].start()
    for write in writes:
        write.wait()


def program(heat, cotan, source_index):
    peers, senders = lax.axis_size("vtx"), lax.axis_size("src")
    all_sources, own_rows, width = heat.shape
    rows_dev = cotan.shape[1]
    total_rows = rows_dev * peers
    group = all_sources // senders
    cb = width // LANES
    amplitude = math.sqrt(total_rows * width) / 8.0
    me = lax.axis_index("src")
    view = heat.reshape(all_sources, own_rows, cb, LANES).transpose(0, 2, 1, 3).reshape(-1, LANES)
    outer_rows = (0, own_rows - 1)
    order = [k for k in range(1, senders) if k >= 2] + [1]
    halves = [(0, group // 2), (group // 2, group - group // 2)]
    chunks = [(0, group - group // 4), (group - group // 4, group // 4)]
    common = (group, cb, own_rows, senders)

    def send(k, piece):
        return lax.ppermute(piece, "src", [(i, i ^ k) for i in range(senders)]) if k else piece

    first_wanted = [(k, outer_rows, *halves[0]) for k in order[:-1]]
    wanted = [(k, outer_rows, *halves[1]) for k in order]
    wanted += [(k, outer_rows, *halves[0]) for k in (1, 0)] + [(0, outer_rows, *halves[1])]
    wanted += [(k, (1 + j, j), *chunk) for chunk in chunks for j in range(own_rows - 1) for k in order + [0]]
    packed = pack(view, first_wanted, [(k, *halves[0]) for k in order[:-1]], *common, 60)
    table = dict(zip(first_wanted, packed, strict=True))
    packed = pack(view, wanted, [(k, *half) for half in reversed(halves) for k in order + [0]], *common, 16)
    table.update(zip(wanted, packed, strict=True))
    for key, piece in table.items():
        table[key] = send(key[0], piece)
    outer = [{k: table[k, outer_rows, *half] for k in range(senders)} for half in halves]
    inner = [
        [{k: table[k, (1 + j, j), *chunk] for k in range(senders)} for j in range(own_rows - 1)] for chunk in chunks
    ]
    up = [(i, i + 1) for i in range(peers - 1)]
    down = [(j, i) for i, j in up]
    vmem = pl.BlockSpec(memory_space=pltpu.VMEM)
    smem = pl.BlockSpec(memory_space=pltpu.SMEM)
    per = cb * rows_dev
    lower = lax.ppermute(cotan[2:4, rows_dev - 1].reshape(2 * cb, LANES), "vtx", up)
    tiles = cotan.reshape(4, rows_dev, cb, LANES).transpose(0, 2, 1, 3).reshape(4 * per, LANES)
    weights = pl.pallas_call(
        functools.partial(weights_kernel, (rows_dev, cb, total_rows)),
        out_shape=jax.ShapeDtypeStruct((7, rows_dev, cb + PAD, LANES), jnp.float32),
        in_specs=[vmem, vmem],
        out_specs=vmem,
        compiler_params=pltpu.CompilerParams(vmem_limit_bytes=8 << 20),
        cost_estimate=pl.CostEstimate(flops=20 * per * LANES, bytes_accessed=44 * per * LANES, transcendentals=0),
        name="weights",
    )(tiles, lower)
    below, above = [], []
    for got in outer:
        first = lax.select_n(me, *[got[k] for k in range(senders)])
        last = lax.select_n(me, *[got[k] for k in reversed(range(senders))])
        above.append(lax.ppermute(first, "vtx", down))
        below.append(lax.ppermute(last, "vtx", up))

    parts, sums = [], None
    for c, (lo, n) in enumerate(chunks):
        pieces, ins = [], []

        def take(kind, k, first, count, array):
            begin, end = max(first, lo), min(first + count, lo + n)
            if begin < end:
                pieces.append((kind, k, begin, end - begin, begin - first))
                ins.append(array)

        for half, got, b, a in zip(halves, outer, below, above, strict=True):
            for k in range(senders):
                take("outer", k, *half, got[k])
            take("below", 0, *half, b)
            take("above", 0, *half, a)
        for j in range(own_rows - 1):
            for k in range(senders):
                take(j, k, lo, n, inner[c][j][k])
        meta = (tuple(pieces), rows_dev, cb, senders, own_rows)
        part, sums = pl.pallas_call(
            functools.partial(defect_kernel, meta, lo, n, group, amplitude),
            out_shape=(
                jax.ShapeDtypeStruct((n * per, LANES), jnp.float32),
                jax.ShapeDtypeStruct((group, LANES), jnp.float32),
            ),
            in_specs=[smem, vmem] + [vmem] * len(ins) + ([vmem] if lo else []),
            out_specs=(vmem, vmem),
            scratch_shapes=[
                pltpu.VMEM((rows_dev + 2, n * cb + PAD + TAIL, LANES), jnp.float32),
            ],
            cost_estimate=pl.CostEstimate(flops=20 * n * per * LANES, bytes_accessed=8 * n * per * LANES, transcendentals=0),
            compiler_params=pltpu.CompilerParams(vmem_limit_bytes=24 << 20),
            name="defect",
        )(source_index, weights, *ins, *([sums] if lo else []))
        parts.append(part)
    step, other = 1, None
    while step < peers:
        sums = sums if other is None else sums + other
        other = lax.ppermute(sums, "vtx", [(i, i ^ step) for i in range(peers)])
        step *= 2
    out, norms = pl.pallas_call(
        functools.partial(scale_kernel, chunks, float(total_rows * width)),
        out_shape=(
            jax.ShapeDtypeStruct((group * per, LANES), jnp.float32),
            jax.ShapeDtypeStruct((1, group), jnp.float32),
        ),
        in_specs=[vmem, vmem] + [vmem] * len(parts),
        out_specs=(pl.BlockSpec(memory_space=pltpu.HBM), vmem),
        scratch_shapes=[
            pltpu.VMEM((group * per, LANES), jnp.float32),
            pltpu.SemaphoreType.DMA((group,)),
        ],
        cost_estimate=pl.CostEstimate(flops=group * per * LANES, bytes_accessed=8 * group * per * LANES, transcendentals=0),
        compiler_params=pltpu.CompilerParams(vmem_limit_bytes=12 << 20),
        name="scale",
    )(sums, other, *parts)
    out = out.reshape(group, cb, rows_dev, LANES).transpose(0, 2, 1, 3).reshape(group, rows_dev, width)
    return out, norms.reshape(group)


def solution(mesh):
    return jax.shard_map(
        program,
        mesh=mesh,
        in_specs=(P(None, ("vtx", "src"), None), P(None, "vtx", None), P()),
        out_specs=(P("src", "vtx", None), P("src")),
        check_vma=False,
    )
```

```python
import functools
import math

import jax
import jax.numpy as jnp
from jax import lax
from jax.experimental import pallas as pl
from jax.experimental.pallas import tpu as pltpu
from jax.sharding import PartitionSpec as P


LANES = 128
SUB = 8
PAD = 8
TAIL = 16


def pack_kernel(meta, heat, *refs):
    blocks, group, cb, own_rows, senders = meta
    n_out = max(out for *_, targets in blocks for out, *_ in targets) + 1
    outs = refs[:n_out]
    wide, in_sem = refs[n_out:]
    me = lax.axis_index("src")
    low = me < senders // 2
    reads, at = [], 0
    for b, (k, lo, n, _) in enumerate(blocks):
        size = n * cb * own_rows
        copy = pltpu.make_async_copy(
            heat.at[pl.ds(((me ^ k) * group + lo) * cb * own_rows, size), :], wide.at[pl.ds(at, size), :], in_sem.at[b]
        )
        copy.start()
        reads.append((copy, at))
        at += size
    for (copy, at), (k, lo, n, targets) in zip(reads, blocks, strict=True):
        copy.wait()
        for out, rows, skip, first, count in targets:
            start = at + skip * cb * own_rows + jnp.where(low, rows[0], rows[1])

            def step(i, _, start=start, ref=outs[out], first=first):
                for u in range(cb // SUB):
                    to = pl.multiple_of((first + i) * cb + u * SUB, SUB)
                    ref[pl.ds(to, SUB), :] = wide[pl.ds(start + (i * cb + u * SUB) * own_rows, SUB, stride=own_rows), :]
                return 0

            lax.fori_loop(0, count, step, 0)


def pack(heat, wanted, blocks, group, cb, own_rows, senders, limit):
    plan = []
    for k, lo, n in blocks:
        targets = []
        for out, (wk, rows, first, count) in enumerate(wanted):
            begin, end = max(lo, first), min(lo + n, first + count)
            if wk == k and begin < end:
                targets.append((out, rows, begin - lo, begin - first, end - begin))
        plan.append((k, lo, n, tuple(targets)))
    reads = sum(n for _, n in ((k, n) for k, _, n in blocks)) * cb * own_rows
    writes = sum(count for *_, count in wanted) * cb
    vmem = pl.BlockSpec(memory_space=pltpu.VMEM)
    return pl.pallas_call(
        functools.partial(pack_kernel, (tuple(plan), group, cb, own_rows, senders)),
        out_shape=tuple(jax.ShapeDtypeStruct((count * cb, LANES), jnp.float32) for *_, count in wanted),
        in_specs=[pl.BlockSpec(memory_space=pltpu.HBM)],
        out_specs=tuple(vmem for _ in wanted),
        scratch_shapes=[
            pltpu.VMEM((reads, LANES), jnp.float32),
            pltpu.SemaphoreType.DMA((len(blocks),)),
        ],
        compiler_params=pltpu.CompilerParams(vmem_limit_bytes=limit << 20),
        cost_estimate=pl.CostEstimate(flops=writes * LANES, bytes_accessed=4 * (reads + writes) * LANES, transcendentals=0),
    )(heat)


def weights_kernel(meta, cotan, lower, out):
    rows_dev, cb, total_rows = meta
    block_start = lax.axis_index("vtx") * rows_dev
    lane = lax.broadcasted_iota(jnp.int32, (SUB, LANES), 1)
    index = lax.broadcasted_iota(jnp.int32, (SUB, LANES), 0) * LANES + lane
    last_lane = lane == LANES - 1

    def column_step(q, _):
        at = pl.ds(pl.multiple_of(q * SUB, SUB), SUB)
        inside_left = index + q * SUB * LANES > 0
        inside_right = index + q * SUB * LANES < cb * LANES - 1

        def row_of(array, row, back=0):
            return cotan[pl.ds((array * cb + q * SUB - back) * rows_dev + row, SUB, stride=rows_dev), :]

        def from_left(value, before):
            moved = pltpu.roll(jnp.where(last_lane, before, value), 1, 1)
            return jnp.where(inside_left, moved, 0.0)

        south = lower[pl.ds(pl.multiple_of(q * SUB, SUB), SUB), :]
        southwest = from_left(
            lower[pl.ds(pl.multiple_of(cb + q * SUB, SUB), SUB), :], lower[pl.ds(cb - 1 + q * SUB, SUB), :]
        )
        for row in range(rows_dev):
            inside_row = jnp.full((SUB, LANES), block_start + row, jnp.int32) < total_rows - 1
            east = row_of(1, row)
            west = from_left(east, row_of(1, row, 1))
            east = jnp.where(inside_right, east, 0.0)
            north = jnp.where(inside_row, row_of(2, row), 0.0)
            raw = row_of(3, row)
            diag = jnp.where(inside_right & inside_row, raw, 0.0)
            centre = row_of(0, row) + east + west + north + south + diag + southwest
            for w, value in enumerate((centre, east, west, north, south, diag, southwest)):
                out[w, row, at, :] = value
            south, southwest = north, from_left(raw, row_of(3, row, 1))
        return 0

    lax.fori_loop(0, cb // SUB, column_step, 0)


def defect_kernel(meta, lo, n, group, amplitude, *refs):
    pieces, rows_dev, cb, senders, own_rows = meta
    n_in = len(pieces)
    sources, weights = refs[:2]
    ins = refs[2 : 2 + n_in]
    prev = refs[2 + n_in] if lo else None
    out, sums, grid = refs[-3:]
    me = lax.axis_index("src")
    for ref, (kind, k, first, count, skip) in zip(ins, pieces, strict=True):
        t = me ^ k
        low = t < senders // 2
        if kind == "below":
            row = 0
        elif kind == "above":
            row = rows_dev + 1
        elif kind == "outer":
            row = 1 + t * own_rows + jnp.where(low, 0, own_rows - 1)
        else:
            row = 1 + t * own_rows + kind + jnp.where(low, 1, 0)

        def move(i, _, ref=ref, row=row, first=first, skip=skip):
            for u in range(cb // SUB):
                to = pl.multiple_of(PAD + (first - lo + i) * cb + u * SUB, SUB)
                grid[row, pl.ds(to, SUB), :] = ref[pl.ds(pl.multiple_of((skip + i) * cb + u * SUB, SUB), SUB), :]
            return 0

        lax.fori_loop(0, count, move, 0)
    zero = jnp.zeros((SUB, LANES), jnp.float32)
    for row in range(rows_dev + 2):
        grid[row, pl.ds(0, PAD), :] = zero
        grid[row, pl.ds(PAD + n * cb, PAD), :] = zero
    if lo:
        sums[...] = prev[...]
    else:
        sums[...] = jnp.zeros(sums.shape, jnp.float32)
    lane = lax.broadcasted_iota(jnp.int32, (SUB, LANES), 1)
    index = lax.broadcasted_iota(jnp.int32, (SUB, LANES), 0) * LANES + lane
    first_lane, last_lane = lane == 0, lane == LANES - 1
    width = cb * LANES
    start = lax.axis_index("vtx") * rows_dev * width

    def source_step(i, _):
        source = sources[me * group + lo + i] - start

        def column_step(q, total):
            base = pl.multiple_of(PAD + i * cb + q * SUB, SUB)
            at = pl.ds(pl.multiple_of(q * SUB, SUB), SUB)
            here, right, left = [], [], []
            for row in range(rows_dev + 2):
                value = grid[row, pl.ds(base, SUB), :]
                here.append(value)
                after = grid[row, pl.ds(base + 1, SUB), :] if row else None
                right.append(pltpu.roll(jnp.where(first_lane, after, value), LANES - 1, 1) if row else None)
                if row <= rows_dev:
                    before = grid[row, pl.ds(base - 1, SUB), :]
                    left.append(pltpu.roll(jnp.where(last_lane, before, value), 1, 1))
            for row in range(rows_dev):
                c = [weights[w, row, at, :] for w in range(7)]
                value = c[0] * here[row + 1] - c[1] * right[row + 1] - c[2] * left[row + 1]
                value = value - c[3] * here[row + 2] - c[4] * here[row]
                value = value - c[5] * right[row + 2] - c[6] * left[row]
                spot = source - row * width - q * SUB * LANES
                value = value - jnp.where(index == spot, amplitude, 0.0)
                out[pl.ds((i * cb + q * SUB) * rows_dev + row, SUB, stride=rows_dev), :] = value
                total = total + value * value
            return total

        total = lax.fori_loop(0, cb // SUB, column_step, zero, unroll=math.gcd(cb // SUB, 8))
        sums[pl.ds(lo + i, 1), :] = jnp.sum(total, axis=0, keepdims=True)
        return 0

    lax.fori_loop(0, n, source_step, 0)


def scale_kernel(chunks, size, *refs):
    mine, other, parts, out, norms, buf, out_sem = refs[0], refs[1], refs[2:-4], *refs[-4:]
    group, per = mine.shape[0], out.shape[0] // mine.shape[0]
    sums = jnp.sum(mine[...] + other[...], axis=1, keepdims=True)
    norm = jnp.sqrt(sums / size + 1e-06)
    lane = lax.broadcasted_iota(jnp.int32, (group, LANES), 1)
    sub = lax.broadcasted_iota(jnp.int32, (group, LANES), 0)
    spread = jnp.where(lane == sub, jnp.broadcast_to(norm, (group, LANES)), 0.0)
    norms[...] = jnp.sum(spread, axis=0, keepdims=True)[:, :group]
    inverse = jnp.broadcast_to(1.0 / norm, (group, LANES))
    writes = []
    for i in range(group):
        part, (lo, n) = [(p, c) for p, c in zip(parts, chunks, strict=True) if c[0] <= i < sum(c)][0]
        factor = jnp.broadcast_to(inverse[i : i + 1], (SUB, LANES))

        def step(j, _, i=i, lo=lo, part=part, factor=factor):
            for u in range(8):
                at = (j * 8 + u) * SUB
                to = pl.ds(pl.multiple_of(i * per + at, SUB), SUB)
                buf[to, :] = part[pl.ds(pl.multiple_of((i - lo) * per + at, SUB), SUB), :] * factor
            return 0

        lax.fori_loop(0, per // (SUB * 8), step, 0)
        spot = pl.ds(i * per, per)
        writes.append(pltpu.make_async_copy(buf.at[spot, :], out.at[spot, :], out_sem.at[i]))
        writes[-1].start()
    for write in writes:
        write.wait()


def program(heat, cotan, source_index):
    peers, senders = lax.axis_size("vtx"), lax.axis_size("src")
    all_sources, own_rows, width = heat.shape
    rows_dev = cotan.shape[1]
    total_rows = rows_dev * peers
    group = all_sources // senders
    cb = width // LANES
    amplitude = math.sqrt(total_rows * width) / 8.0
    me = lax.axis_index("src")
    view = heat.reshape(all_sources, own_rows, cb, LANES).transpose(0, 2, 1, 3).reshape(-1, LANES)
    outer_rows = (0, own_rows - 1)
    order = [k for k in range(1, senders) if k >= 2] + [1]
    halves = [(0, group // 2), (group // 2, group - group // 2)]
    chunks = [(0, group - group // 4), (group - group // 4, group // 4)]
    common = (group, cb, own_rows, senders)

    def send(k, piece):
        return lax.ppermute(piece, "src", [(i, i ^ k) for i in range(senders)]) if k else piece

    wanted = [(k, outer_rows, *half) for half in halves for k in (1, 0)]
    wanted += [(k, (1 + j, j), *chunk) for chunk in chunks for j in range(own_rows - 1) for k in order + [0]]
    table = {}
    for half in halves:
        early = [(k, outer_rows, *half) for k in order[:-1]]
        packed = pack(view, early, [(k, *half) for k in order[:-1]], *common, 60)
        table.update(zip(early, packed, strict=True))
    packed = pack(view, wanted, [(k, *half) for half in halves for k in order + [0]], *common, 60)
    table.update(zip(wanted, packed, strict=True))
    for key, piece in table.items():
        table[key] = send(key[0], piece)
    outer = [{k: table[k, outer_rows, *half] for k in range(senders)} for half in halves]
    inner = [
        [{k: table[k, (1 + j, j), *chunk] for k in range(senders)} for j in range(own_rows - 1)] for chunk in chunks
    ]
    up = [(i, i + 1) for i in range(peers - 1)]
    down = [(j, i) for i, j in up]
    vmem = pl.BlockSpec(memory_space=pltpu.VMEM)
    smem = pl.BlockSpec(memory_space=pltpu.SMEM)
    per = cb * rows_dev
    lower = lax.ppermute(cotan[2:4, rows_dev - 1].reshape(2 * cb, LANES), "vtx", up)
    tiles = cotan.reshape(4, rows_dev, cb, LANES).transpose(0, 2, 1, 3).reshape(4 * per, LANES)
    weights = pl.pallas_call(
        functools.partial(weights_kernel, (rows_dev, cb, total_rows)),
        out_shape=jax.ShapeDtypeStruct((7, rows_dev, cb + PAD, LANES), jnp.float32),
        in_specs=[vmem, vmem],
        out_specs=vmem,
        compiler_params=pltpu.CompilerParams(vmem_limit_bytes=8 << 20),
        cost_estimate=pl.CostEstimate(flops=20 * per * LANES, bytes_accessed=44 * per * LANES, transcendentals=0),
        name="weights",
    )(tiles, lower)
    below, above = [], []
    for got in outer:
        first = lax.select_n(me, *[got[k] for k in range(senders)])
        last = lax.select_n(me, *[got[k] for k in reversed(range(senders))])
        above.append(lax.ppermute(first, "vtx", down))
        below.append(lax.ppermute(last, "vtx", up))

    parts, sums = [], None
    for c, (lo, n) in enumerate(chunks):
        pieces, ins = [], []

        def take(kind, k, first, count, array):
            begin, end = max(first, lo), min(first + count, lo + n)
            if begin < end:
                pieces.append((kind, k, begin, end - begin, begin - first))
                ins.append(array)

        for half, got, b, a in zip(halves, outer, below, above, strict=True):
            for k in range(senders):
                take("outer", k, *half, got[k])
            take("below", 0, *half, b)
            take("above", 0, *half, a)
        for j in range(own_rows - 1):
            for k in range(senders):
                take(j, k, lo, n, inner[c][j][k])
        meta = (tuple(pieces), rows_dev, cb, senders, own_rows)
        part, sums = pl.pallas_call(
            functools.partial(defect_kernel, meta, lo, n, group, amplitude),
            out_shape=(
                jax.ShapeDtypeStruct((n * per, LANES), jnp.float32),
                jax.ShapeDtypeStruct((group, LANES), jnp.float32),
            ),
            in_specs=[smem, vmem] + [vmem] * len(ins) + ([vmem] if lo else []),
            out_specs=(vmem, vmem),
            scratch_shapes=[
                pltpu.VMEM((rows_dev + 2, n * cb + PAD + TAIL, LANES), jnp.float32),
            ],
            cost_estimate=pl.CostEstimate(flops=20 * n * per * LANES, bytes_accessed=8 * n * per * LANES, transcendentals=0),
            compiler_params=pltpu.CompilerParams(vmem_limit_bytes=24 << 20),
            name="defect",
        )(source_index, weights, *ins, *([sums] if lo else []))
        parts.append(part)
    step, other = 1, None
    while step < peers:
        sums = sums if other is None else sums + other
        other = lax.ppermute(sums, "vtx", [(i, i ^ step) for i in range(peers)])
        step *= 2
    out, norms = pl.pallas_call(
        functools.partial(scale_kernel, chunks, float(total_rows * width)),
        out_shape=(
            jax.ShapeDtypeStruct((group * per, LANES), jnp.float32),
            jax.ShapeDtypeStruct((1, group), jnp.float32),
        ),
        in_specs=[vmem, vmem] + [vmem] * len(parts),
        out_specs=(pl.BlockSpec(memory_space=pltpu.HBM), vmem),
        scratch_shapes=[
            pltpu.VMEM((group * per, LANES), jnp.float32),
            pltpu.SemaphoreType.DMA((group,)),
        ],
        cost_estimate=pl.CostEstimate(flops=group * per * LANES, bytes_accessed=8 * group * per * LANES, transcendentals=0),
        compiler_params=pltpu.CompilerParams(vmem_limit_bytes=12 << 20),
        name="scale",
    )(sums, other, *parts)
    out = out.reshape(group, cb, rows_dev, LANES).transpose(0, 2, 1, 3).reshape(group, rows_dev, width)
    return out, norms.reshape(group)


def solution(mesh):
    return jax.shard_map(
        program,
        mesh=mesh,
        in_specs=(P(None, ("vtx", "src"), None), P(None, "vtx", None), P()),
        out_specs=(P("src", "vtx", None), P("src")),
        check_vma=False,
    )
```

```python
import functools
import math

import jax
import jax.numpy as jnp
from jax import lax
from jax.experimental import pallas as pl
from jax.experimental.pallas import tpu as pltpu
from jax.sharding import PartitionSpec as P


LANES = 128
SUB = 8
PAD = 8
TAIL = 16


def pack_kernel(meta, heat, *refs):
    blocks, group, cb, own_rows, senders = meta
    n_out = max(out for *_, targets in blocks for out, *_ in targets) + 1
    outs = refs[:n_out]
    wide, in_sem = refs[n_out:]
    me = lax.axis_index("src")
    low = me < senders // 2
    reads, at = [], 0
    for b, (k, lo, n, _) in enumerate(blocks):
        size = n * cb * own_rows
        copy = pltpu.make_async_copy(
            heat.at[pl.ds(((me ^ k) * group + lo) * cb * own_rows, size), :], wide.at[pl.ds(at, size), :], in_sem.at[b]
        )
        copy.start()
        reads.append((copy, at))
        at += size
    for (copy, at), (k, lo, n, targets) in zip(reads, blocks, strict=True):
        copy.wait()
        for out, rows, skip, first, count in targets:
            start = at + skip * cb * own_rows + jnp.where(low, rows[0], rows[1])

            def step(i, _, start=start, ref=outs[out], first=first):
                for u in range(cb // SUB):
                    to = pl.multiple_of((first + i) * cb + u * SUB, SUB)
                    ref[pl.ds(to, SUB), :] = wide[pl.ds(start + (i * cb + u * SUB) * own_rows, SUB, stride=own_rows), :]
                return 0

            lax.fori_loop(0, count, step, 0)


def pack(heat, wanted, blocks, group, cb, own_rows, senders, limit):
    plan = []
    for k, lo, n in blocks:
        targets = []
        for out, (wk, rows, first, count) in enumerate(wanted):
            begin, end = max(lo, first), min(lo + n, first + count)
            if wk == k and begin < end:
                targets.append((out, rows, begin - lo, begin - first, end - begin))
        plan.append((k, lo, n, tuple(targets)))
    reads = sum(n for _, n in ((k, n) for k, _, n in blocks)) * cb * own_rows
    writes = sum(count for *_, count in wanted) * cb
    vmem = pl.BlockSpec(memory_space=pltpu.VMEM)
    return pl.pallas_call(
        functools.partial(pack_kernel, (tuple(plan), group, cb, own_rows, senders)),
        out_shape=tuple(jax.ShapeDtypeStruct((count * cb, LANES), jnp.float32) for *_, count in wanted),
        in_specs=[pl.BlockSpec(memory_space=pltpu.HBM)],
        out_specs=tuple(vmem for _ in wanted),
        scratch_shapes=[
            pltpu.VMEM((reads, LANES), jnp.float32),
            pltpu.SemaphoreType.DMA((len(blocks),)),
        ],
        compiler_params=pltpu.CompilerParams(vmem_limit_bytes=limit << 20),
        cost_estimate=pl.CostEstimate(flops=writes * LANES, bytes_accessed=4 * (reads + writes) * LANES, transcendentals=0),
    )(heat)


def weights_kernel(meta, cotan, lower, out):
    rows_dev, cb, total_rows = meta
    block_start = lax.axis_index("vtx") * rows_dev
    lane = lax.broadcasted_iota(jnp.int32, (SUB, LANES), 1)
    index = lax.broadcasted_iota(jnp.int32, (SUB, LANES), 0) * LANES + lane
    last_lane = lane == LANES - 1

    def column_step(q, _):
        at = pl.ds(pl.multiple_of(q * SUB, SUB), SUB)
        inside_left = index + q * SUB * LANES > 0
        inside_right = index + q * SUB * LANES < cb * LANES - 1

        def row_of(array, row, back=0):
            return cotan[pl.ds((array * cb + q * SUB - back) * rows_dev + row, SUB, stride=rows_dev), :]

        def from_left(value, before):
            moved = pltpu.roll(jnp.where(last_lane, before, value), 1, 1)
            return jnp.where(inside_left, moved, 0.0)

        south = lower[pl.ds(pl.multiple_of(q * SUB, SUB), SUB), :]
        southwest = from_left(
            lower[pl.ds(pl.multiple_of(cb + q * SUB, SUB), SUB), :], lower[pl.ds(cb - 1 + q * SUB, SUB), :]
        )
        for row in range(rows_dev):
            inside_row = jnp.full((SUB, LANES), block_start + row, jnp.int32) < total_rows - 1
            east = row_of(1, row)
            west = from_left(east, row_of(1, row, 1))
            east = jnp.where(inside_right, east, 0.0)
            north = jnp.where(inside_row, row_of(2, row), 0.0)
            raw = row_of(3, row)
            diag = jnp.where(inside_right & inside_row, raw, 0.0)
            centre = row_of(0, row) + east + west + north + south + diag + southwest
            for w, value in enumerate((centre, east, west, north, south, diag, southwest)):
                out[w, row, at, :] = value
            south, southwest = north, from_left(raw, row_of(3, row, 1))
        return 0

    lax.fori_loop(0, cb // SUB, column_step, 0)


def defect_kernel(meta, lo, n, group, amplitude, *refs):
    pieces, rows_dev, cb, senders, own_rows = meta
    n_in = len(pieces)
    sources, weights = refs[:2]
    ins = refs[2 : 2 + n_in]
    prev = refs[2 + n_in] if lo else None
    out, sums, grid = refs[-3:]
    me = lax.axis_index("src")
    for ref, (kind, k, first, count, skip) in zip(ins, pieces, strict=True):
        t = me ^ k
        low = t < senders // 2
        if kind == "below":
            row = 0
        elif kind == "above":
            row = rows_dev + 1
        elif kind == "outer":
            row = 1 + t * own_rows + jnp.where(low, 0, own_rows - 1)
        else:
            row = 1 + t * own_rows + kind + jnp.where(low, 1, 0)

        def move(i, _, ref=ref, row=row, first=first, skip=skip):
            for u in range(cb // SUB):
                to = pl.multiple_of(PAD + (first - lo + i) * cb + u * SUB, SUB)
                grid[row, pl.ds(to, SUB), :] = ref[pl.ds(pl.multiple_of((skip + i) * cb + u * SUB, SUB), SUB), :]
            return 0

        lax.fori_loop(0, count, move, 0)
    zero = jnp.zeros((SUB, LANES), jnp.float32)
    for row in range(rows_dev + 2):
        grid[row, pl.ds(0, PAD), :] = zero
        grid[row, pl.ds(PAD + n * cb, PAD), :] = zero
    if lo:
        sums[...] = prev[...]
    else:
        sums[...] = jnp.zeros(sums.shape, jnp.float32)
    lane = lax.broadcasted_iota(jnp.int32, (SUB, LANES), 1)
    index = lax.broadcasted_iota(jnp.int32, (SUB, LANES), 0) * LANES + lane
    first_lane, last_lane = lane == 0, lane == LANES - 1
    width = cb * LANES
    start = lax.axis_index("vtx") * rows_dev * width

    def source_step(i, _):
        source = sources[me * group + lo + i] - start

        def column_step(q, total):
            base = pl.multiple_of(PAD + i * cb + q * SUB, SUB)
            at = pl.ds(pl.multiple_of(q * SUB, SUB), SUB)
            here, right, left = [], [], []
            for row in range(rows_dev + 2):
                value = grid[row, pl.ds(base, SUB), :]
                here.append(value)
                after = grid[row, pl.ds(base + 1, SUB), :] if row else None
                right.append(pltpu.roll(jnp.where(first_lane, after, value), LANES - 1, 1) if row else None)
                if row <= rows_dev:
                    before = grid[row, pl.ds(base - 1, SUB), :]
                    left.append(pltpu.roll(jnp.where(last_lane, before, value), 1, 1))
            for row in range(rows_dev):
                c = [weights[w, row, at, :] for w in range(7)]
                value = c[0] * here[row + 1] - c[1] * right[row + 1] - c[2] * left[row + 1]
                value = value - c[3] * here[row + 2] - c[4] * here[row]
                value = value - c[5] * right[row + 2] - c[6] * left[row]
                spot = source - row * width - q * SUB * LANES
                value = value - jnp.where(index == spot, amplitude, 0.0)
                out[pl.ds((i * cb + q * SUB) * rows_dev + row, SUB, stride=rows_dev), :] = value
                total = total + value * value
            return total

        total = lax.fori_loop(0, cb // SUB, column_step, zero, unroll=math.gcd(cb // SUB, 8))
        sums[pl.ds(lo + i, 1), :] = jnp.sum(total, axis=0, keepdims=True)
        return 0

    lax.fori_loop(0, n, source_step, 0)


def scale_kernel(chunks, size, *refs):
    mine, other, parts, out, norms, buf, out_sem = refs[0], refs[1], refs[2:-4], *refs[-4:]
    group, per = mine.shape[0], out.shape[0] // mine.shape[0]
    sums = jnp.sum(mine[...] + other[...], axis=1, keepdims=True)
    norm = jnp.sqrt(sums / size + 1e-06)
    lane = lax.broadcasted_iota(jnp.int32, (group, LANES), 1)
    sub = lax.broadcasted_iota(jnp.int32, (group, LANES), 0)
    spread = jnp.where(lane == sub, jnp.broadcast_to(norm, (group, LANES)), 0.0)
    norms[...] = jnp.sum(spread, axis=0, keepdims=True)[:, :group]
    buf[pl.ds(group * per, group), :] = jnp.broadcast_to(1.0 / norm, (group, LANES))

    def copy_of(i):
        spot = pl.ds(pl.multiple_of(i * per, per), per)
        return pltpu.make_async_copy(buf.at[spot, :], out.at[spot, :], out_sem.at[i])

    for part, (lo, n) in zip(parts, chunks, strict=True):

        def step(i, _, part=part, lo=lo):
            factor = jnp.broadcast_to(buf[pl.ds(group * per + lo + i, 1), :], (SUB, LANES))
            for at in range(0, per, SUB):
                to = pl.ds(pl.multiple_of((lo + i) * per + at, SUB), SUB)
                buf[to, :] = part[pl.ds(pl.multiple_of(i * per + at, SUB), SUB), :] * factor
            copy_of(lo + i).start()
            return 0

        lax.fori_loop(0, n, step, 0)

    def finish(i, _):
        copy_of(i).wait()
        return 0

    lax.fori_loop(0, group, finish, 0)


def program(heat, cotan, source_index):
    peers, senders = lax.axis_size("vtx"), lax.axis_size("src")
    all_sources, own_rows, width = heat.shape
    rows_dev = cotan.shape[1]
    total_rows = rows_dev * peers
    group = all_sources // senders
    cb = width // LANES
    amplitude = math.sqrt(total_rows * width) / 8.0
    me = lax.axis_index("src")
    view = heat.reshape(all_sources, own_rows, cb, LANES).transpose(0, 2, 1, 3).reshape(-1, LANES)
    outer_rows = (0, own_rows - 1)
    order = [k for k in range(1, senders) if k >= 2] + [1]
    halves = [(0, group // 2), (group // 2, group - group // 2)]
    chunks = [(0, group - group // 4), (group - group // 4, group // 4)]
    common = (group, cb, own_rows, senders)

    def send(k, piece):
        return lax.ppermute(piece, "src", [(i, i ^ k) for i in range(senders)]) if k else piece

    wanted = [(k, outer_rows, *half) for half in halves for k in (1, 0)]
    wanted += [(k, (1 + j, j), *chunk) for chunk in chunks for j in range(own_rows - 1) for k in order + [0]]
    table = {}
    for half in halves:
        early = [(k, outer_rows, *half) for k in order[:-1]]
        packed = pack(view, early, [(k, *half) for k in order[:-1]], *common, 60)
        table.update(zip(early, packed, strict=True))
    packed = pack(view, wanted, [(k, *half) for half in halves for k in order + [0]], *common, 60)
    table.update(zip(wanted, packed, strict=True))
    for key, piece in table.items():
        table[key] = send(key[0], piece)
    outer = [{k: table[k, outer_rows, *half] for k in range(senders)} for half in halves]
    inner = [
        [{k: table[k, (1 + j, j), *chunk] for k in range(senders)} for j in range(own_rows - 1)] for chunk in chunks
    ]
    up = [(i, i + 1) for i in range(peers - 1)]
    down = [(j, i) for i, j in up]
    vmem = pl.BlockSpec(memory_space=pltpu.VMEM)
    smem = pl.BlockSpec(memory_space=pltpu.SMEM)
    per = cb * rows_dev
    lower = lax.ppermute(cotan[2:4, rows_dev - 1].reshape(2 * cb, LANES), "vtx", up)
    tiles = cotan.reshape(4, rows_dev, cb, LANES).transpose(0, 2, 1, 3).reshape(4 * per, LANES)
    weights = pl.pallas_call(
        functools.partial(weights_kernel, (rows_dev, cb, total_rows)),
        out_shape=jax.ShapeDtypeStruct((7, rows_dev, cb + PAD, LANES), jnp.float32),
        in_specs=[vmem, vmem],
        out_specs=vmem,
        compiler_params=pltpu.CompilerParams(vmem_limit_bytes=8 << 20),
        cost_estimate=pl.CostEstimate(flops=20 * per * LANES, bytes_accessed=44 * per * LANES, transcendentals=0),
        name="weights",
    )(tiles, lower)
    below, above = [], []
    for got in outer:
        first = lax.select_n(me, *[got[k] for k in range(senders)])
        last = lax.select_n(me, *[got[k] for k in reversed(range(senders))])
        above.append(lax.ppermute(first, "vtx", down))
        below.append(lax.ppermute(last, "vtx", up))

    parts, sums = [], None
    for c, (lo, n) in enumerate(chunks):
        pieces, ins = [], []

        def take(kind, k, first, count, array):
            begin, end = max(first, lo), min(first + count, lo + n)
            if begin < end:
                pieces.append((kind, k, begin, end - begin, begin - first))
                ins.append(array)

        for half, got, b, a in zip(halves, outer, below, above, strict=True):
            for k in range(senders):
                take("outer", k, *half, got[k])
            take("below", 0, *half, b)
            take("above", 0, *half, a)
        for j in range(own_rows - 1):
            for k in range(senders):
                take(j, k, lo, n, inner[c][j][k])
        meta = (tuple(pieces), rows_dev, cb, senders, own_rows)
        part, sums = pl.pallas_call(
            functools.partial(defect_kernel, meta, lo, n, group, amplitude),
            out_shape=(
                jax.ShapeDtypeStruct((n * per, LANES), jnp.float32),
                jax.ShapeDtypeStruct((group, LANES), jnp.float32),
            ),
            in_specs=[smem, vmem] + [vmem] * len(ins) + ([vmem] if lo else []),
            out_specs=(vmem, vmem),
            scratch_shapes=[
                pltpu.VMEM((rows_dev + 2, n * cb + PAD + TAIL, LANES), jnp.float32),
            ],
            cost_estimate=pl.CostEstimate(flops=20 * n * per * LANES, bytes_accessed=8 * n * per * LANES, transcendentals=0),
            compiler_params=pltpu.CompilerParams(vmem_limit_bytes=24 << 20),
            name="defect",
        )(source_index, weights, *ins, *([sums] if lo else []))
        parts.append(part)
    step, other = 1, None
    while step < peers:
        sums = sums if other is None else sums + other
        other = lax.ppermute(sums, "vtx", [(i, i ^ step) for i in range(peers)])
        step *= 2
    out, norms = pl.pallas_call(
        functools.partial(scale_kernel, chunks, float(total_rows * width)),
        out_shape=(
            jax.ShapeDtypeStruct((group * per, LANES), jnp.float32),
            jax.ShapeDtypeStruct((1, group), jnp.float32),
        ),
        in_specs=[vmem, vmem] + [vmem] * len(parts),
        out_specs=(pl.BlockSpec(memory_space=pltpu.HBM), vmem),
        scratch_shapes=[
            pltpu.VMEM((group * per + group, LANES), jnp.float32),
            pltpu.SemaphoreType.DMA((group,)),
        ],
        cost_estimate=pl.CostEstimate(flops=group * per * LANES, bytes_accessed=8 * group * per * LANES, transcendentals=0),
        compiler_params=pltpu.CompilerParams(vmem_limit_bytes=12 << 20),
        name="scale",
    )(sums, other, *parts)
    out = out.reshape(group, cb, rows_dev, LANES).transpose(0, 2, 1, 3).reshape(group, rows_dev, width)
    return out, norms.reshape(group)


def solution(mesh):
    return jax.shard_map(
        program,
        mesh=mesh,
        in_specs=(P(None, ("vtx", "src"), None), P(None, "vtx", None), P()),
        out_specs=(P("src", "vtx", None), P("src")),
        check_vma=False,
    )
```

```python
import functools
import math

import jax
import jax.numpy as jnp
from jax import lax
from jax.experimental import pallas as pl
from jax.experimental.pallas import tpu as pltpu
from jax.sharding import PartitionSpec as P


LANES = 128
SUB = 8
PAD = 8
TAIL = 16


def pack_kernel(meta, heat, *refs):
    blocks, group, cb, own_rows, senders = meta
    n_out = max(out for *_, targets in blocks for out, *_ in targets) + 1
    outs = refs[:n_out]
    wide, in_sem = refs[n_out:]
    me = lax.axis_index("src")
    low = me < senders // 2
    reads, at = [], 0
    for b, (k, lo, n, _) in enumerate(blocks):
        size = n * cb * own_rows
        copy = pltpu.make_async_copy(
            heat.at[pl.ds(((me ^ k) * group + lo) * cb * own_rows, size), :], wide.at[pl.ds(at, size), :], in_sem.at[b]
        )
        copy.start()
        reads.append((copy, at))
        at += size
    for (copy, at), (k, lo, n, targets) in zip(reads, blocks, strict=True):
        copy.wait()
        for out, rows, skip, first, count in targets:
            start = at + skip * cb * own_rows + jnp.where(low, rows[0], rows[1])

            def step(i, _, start=start, ref=outs[out], first=first):
                for u in range(cb // SUB):
                    to = pl.multiple_of((first + i) * cb + u * SUB, SUB)
                    ref[pl.ds(to, SUB), :] = wide[pl.ds(start + (i * cb + u * SUB) * own_rows, SUB, stride=own_rows), :]
                return 0

            lax.fori_loop(0, count, step, 0)


def pack(heat, wanted, blocks, group, cb, own_rows, senders, limit):
    plan = []
    for k, lo, n in blocks:
        targets = []
        for out, (wk, rows, first, count) in enumerate(wanted):
            begin, end = max(lo, first), min(lo + n, first + count)
            if wk == k and begin < end:
                targets.append((out, rows, begin - lo, begin - first, end - begin))
        plan.append((k, lo, n, tuple(targets)))
    reads = sum(n for _, n in ((k, n) for k, _, n in blocks)) * cb * own_rows
    writes = sum(count for *_, count in wanted) * cb
    vmem = pl.BlockSpec(memory_space=pltpu.VMEM)
    return pl.pallas_call(
        functools.partial(pack_kernel, (tuple(plan), group, cb, own_rows, senders)),
        out_shape=tuple(jax.ShapeDtypeStruct((count * cb, LANES), jnp.float32) for *_, count in wanted),
        in_specs=[pl.BlockSpec(memory_space=pltpu.HBM)],
        out_specs=tuple(vmem for _ in wanted),
        scratch_shapes=[
            pltpu.VMEM((reads, LANES), jnp.float32),
            pltpu.SemaphoreType.DMA((len(blocks),)),
        ],
        compiler_params=pltpu.CompilerParams(vmem_limit_bytes=limit << 20),
        cost_estimate=pl.CostEstimate(flops=writes * LANES, bytes_accessed=4 * (reads + writes) * LANES, transcendentals=0),
    )(heat)


def weights_kernel(meta, cotan, lower, out):
    rows_dev, cb, total_rows = meta
    block_start = lax.axis_index("vtx") * rows_dev
    lane = lax.broadcasted_iota(jnp.int32, (SUB, LANES), 1)
    index = lax.broadcasted_iota(jnp.int32, (SUB, LANES), 0) * LANES + lane
    last_lane = lane == LANES - 1

    def column_step(q, _):
        at = pl.ds(pl.multiple_of(q * SUB, SUB), SUB)
        inside_left = index + q * SUB * LANES > 0
        inside_right = index + q * SUB * LANES < cb * LANES - 1

        def row_of(array, row, back=0):
            return cotan[pl.ds((array * cb + q * SUB - back) * rows_dev + row, SUB, stride=rows_dev), :]

        def from_left(value, before):
            moved = pltpu.roll(jnp.where(last_lane, before, value), 1, 1)
            return jnp.where(inside_left, moved, 0.0)

        south = lower[pl.ds(pl.multiple_of(q * SUB, SUB), SUB), :]
        southwest = from_left(
            lower[pl.ds(pl.multiple_of(cb + q * SUB, SUB), SUB), :], lower[pl.ds(cb - 1 + q * SUB, SUB), :]
        )
        for row in range(rows_dev):
            inside_row = jnp.full((SUB, LANES), block_start + row, jnp.int32) < total_rows - 1
            east = row_of(1, row)
            west = from_left(east, row_of(1, row, 1))
            east = jnp.where(inside_right, east, 0.0)
            north = jnp.where(inside_row, row_of(2, row), 0.0)
            raw = row_of(3, row)
            diag = jnp.where(inside_right & inside_row, raw, 0.0)
            centre = row_of(0, row) + east + west + north + south + diag + southwest
            for w, value in enumerate((centre, east, west, north, south, diag, southwest)):
                out[w, row, at, :] = value
            south, southwest = north, from_left(raw, row_of(3, row, 1))
        return 0

    lax.fori_loop(0, cb // SUB, column_step, 0)


def defect_kernel(meta, lo, n, group, amplitude, *refs):
    pieces, rows_dev, cb, senders, own_rows = meta
    n_in = len(pieces)
    sources, weights = refs[:2]
    ins = refs[2 : 2 + n_in]
    prev = refs[2 + n_in] if lo else None
    out, sums, grid = refs[-3:]
    me = lax.axis_index("src")
    for ref, (kind, k, first, count, skip) in zip(ins, pieces, strict=True):
        t = me ^ k
        low = t < senders // 2
        if kind == "below":
            row = 0
        elif kind == "above":
            row = rows_dev + 1
        elif kind == "outer":
            row = 1 + t * own_rows + jnp.where(low, 0, own_rows - 1)
        else:
            row = 1 + t * own_rows + kind + jnp.where(low, 1, 0)

        def move(i, _, ref=ref, row=row, first=first, skip=skip):
            for u in range(cb // SUB):
                to = pl.multiple_of(PAD + (first - lo + i) * cb + u * SUB, SUB)
                grid[row, pl.ds(to, SUB), :] = ref[pl.ds(pl.multiple_of((skip + i) * cb + u * SUB, SUB), SUB), :]
            return 0

        lax.fori_loop(0, count, move, 0)
    zero = jnp.zeros((SUB, LANES), jnp.float32)
    for row in range(rows_dev + 2):
        grid[row, pl.ds(0, PAD), :] = zero
        grid[row, pl.ds(PAD + n * cb, PAD), :] = zero
    if lo:
        sums[pl.ds(0, group), :] = prev[...]
    else:
        sums[...] = jnp.zeros(sums.shape, jnp.float32)
    lane = lax.broadcasted_iota(jnp.int32, (SUB, LANES), 1)
    index = lax.broadcasted_iota(jnp.int32, (SUB, LANES), 0) * LANES + lane
    first_lane, last_lane = lane == 0, lane == LANES - 1
    width = cb * LANES
    start = lax.axis_index("vtx") * rows_dev * width

    def source_step(i, _):
        source = sources[me * group + lo + i] - start

        def column_step(q, total):
            base = pl.multiple_of(PAD + i * cb + q * SUB, SUB)
            at = pl.ds(pl.multiple_of(q * SUB, SUB), SUB)
            here, right, left = [], [], []
            for row in range(rows_dev + 2):
                value = grid[row, pl.ds(base, SUB), :]
                here.append(value)
                after = grid[row, pl.ds(base + 1, SUB), :] if row else None
                right.append(pltpu.roll(jnp.where(first_lane, after, value), LANES - 1, 1) if row else None)
                if row <= rows_dev:
                    before = grid[row, pl.ds(base - 1, SUB), :]
                    left.append(pltpu.roll(jnp.where(last_lane, before, value), 1, 1))
            for row in range(rows_dev):
                c = [weights[w, row, at, :] for w in range(7)]
                value = c[0] * here[row + 1] - c[1] * right[row + 1] - c[2] * left[row + 1]
                value = value - c[3] * here[row + 2] - c[4] * here[row]
                value = value - c[5] * right[row + 2] - c[6] * left[row]
                spot = source - row * width - q * SUB * LANES
                value = value - jnp.where(index == spot, amplitude, 0.0)
                out[pl.ds((i * cb + q * SUB) * rows_dev + row, SUB, stride=rows_dev), :] = value
                total = total + value * value
            return total

        total = lax.fori_loop(0, cb // SUB, column_step, zero, unroll=math.gcd(cb // SUB, 8))
        sums[pl.ds(lo + i, 1), :] = jnp.sum(total, axis=0, keepdims=True)
        return 0

    lax.fori_loop(0, n, source_step, 0)
    for first in range(group, sums.shape[0], group):
        sums[pl.ds(first, group), :] = sums[pl.ds(0, group), :]


def scale_kernel(chunks, size, *refs):
    total, parts, out, norms, buf, out_sem = refs[0], refs[1:-4], *refs[-4:]
    group = sum(n for _, n in chunks)
    per = out.shape[0] // group
    sums = total[pl.ds(0, group), :]
    for first in range(group, total.shape[0], group):
        sums = sums + total[pl.ds(first, group), :]
    sums = jnp.sum(sums, axis=1, keepdims=True)
    norm = jnp.sqrt(sums / size + 1e-06)
    lane = lax.broadcasted_iota(jnp.int32, (group, LANES), 1)
    sub = lax.broadcasted_iota(jnp.int32, (group, LANES), 0)
    spread = jnp.where(lane == sub, jnp.broadcast_to(norm, (group, LANES)), 0.0)
    norms[...] = jnp.sum(spread, axis=0, keepdims=True)[:, :group]
    buf[pl.ds(group * per, group), :] = jnp.broadcast_to(1.0 / norm, (group, LANES))

    def copy_of(i):
        spot = pl.ds(pl.multiple_of(i * per, per), per)
        return pltpu.make_async_copy(buf.at[spot, :], out.at[spot, :], out_sem.at[i])

    for part, (lo, n) in zip(parts, chunks, strict=True):

        def step(i, _, part=part, lo=lo):
            factor = jnp.broadcast_to(buf[pl.ds(group * per + lo + i, 1), :], (SUB, LANES))
            for at in range(0, per, SUB):
                to = pl.ds(pl.multiple_of((lo + i) * per + at, SUB), SUB)
                buf[to, :] = part[pl.ds(pl.multiple_of(i * per + at, SUB), SUB), :] * factor
            copy_of(lo + i).start()
            return 0

        lax.fori_loop(0, n, step, 0)

    def finish(i, _):
        copy_of(i).wait()
        return 0

    lax.fori_loop(0, group, finish, 0)


def program(heat, cotan, source_index):
    peers, senders = lax.axis_size("vtx"), lax.axis_size("src")
    all_sources, own_rows, width = heat.shape
    rows_dev = cotan.shape[1]
    total_rows = rows_dev * peers
    group = all_sources // senders
    cb = width // LANES
    amplitude = math.sqrt(total_rows * width) / 8.0
    me = lax.axis_index("src")
    view = heat.reshape(all_sources, own_rows, cb, LANES).transpose(0, 2, 1, 3).reshape(-1, LANES)
    outer_rows = (0, own_rows - 1)
    order = [k for k in range(1, senders) if k >= 2] + [1]
    halves = [(0, group // 2), (group // 2, group - group // 2)]
    chunks = [(0, group - group // 4), (group - group // 4, group // 4)]
    common = (group, cb, own_rows, senders)

    def send(k, piece):
        return lax.ppermute(piece, "src", [(i, i ^ k) for i in range(senders)]) if k else piece

    wanted = [(k, outer_rows, *half) for half in halves for k in (1, 0)]
    wanted += [(k, (1 + j, j), *chunk) for chunk in chunks for j in range(own_rows - 1) for k in order + [0]]
    table = {}
    for half in halves:
        early = [(k, outer_rows, *half) for k in order[:-1]]
        packed = pack(view, early, [(k, *half) for k in order[:-1]], *common, 60)
        table.update(zip(early, packed, strict=True))
    packed = pack(view, wanted, [(k, *half) for half in halves for k in order + [0]], *common, 60)
    table.update(zip(wanted, packed, strict=True))
    for key, piece in table.items():
        table[key] = send(key[0], piece)
    outer = [{k: table[k, outer_rows, *half] for k in range(senders)} for half in halves]
    inner = [
        [{k: table[k, (1 + j, j), *chunk] for k in range(senders)} for j in range(own_rows - 1)] for chunk in chunks
    ]
    up = [(i, i + 1) for i in range(peers - 1)]
    down = [(j, i) for i, j in up]
    vmem = pl.BlockSpec(memory_space=pltpu.VMEM)
    smem = pl.BlockSpec(memory_space=pltpu.SMEM)
    per = cb * rows_dev
    lower = lax.ppermute(cotan[2:4, rows_dev - 1].reshape(2 * cb, LANES), "vtx", up)
    tiles = cotan.reshape(4, rows_dev, cb, LANES).transpose(0, 2, 1, 3).reshape(4 * per, LANES)
    weights = pl.pallas_call(
        functools.partial(weights_kernel, (rows_dev, cb, total_rows)),
        out_shape=jax.ShapeDtypeStruct((7, rows_dev, cb + PAD, LANES), jnp.float32),
        in_specs=[vmem, vmem],
        out_specs=vmem,
        compiler_params=pltpu.CompilerParams(vmem_limit_bytes=8 << 20),
        cost_estimate=pl.CostEstimate(flops=20 * per * LANES, bytes_accessed=44 * per * LANES, transcendentals=0),
        name="weights",
    )(tiles, lower)
    below, above = [], []
    for got in outer:
        first = lax.select_n(me, *[got[k] for k in range(senders)])
        last = lax.select_n(me, *[got[k] for k in reversed(range(senders))])
        above.append(lax.ppermute(first, "vtx", down))
        below.append(lax.ppermute(last, "vtx", up))

    parts, sums = [], None
    for c, (lo, n) in enumerate(chunks):
        pieces, ins = [], []

        def take(kind, k, first, count, array):
            begin, end = max(first, lo), min(first + count, lo + n)
            if begin < end:
                pieces.append((kind, k, begin, end - begin, begin - first))
                ins.append(array)

        for half, got, b, a in zip(halves, outer, below, above, strict=True):
            for k in range(senders):
                take("outer", k, *half, got[k])
            take("below", 0, *half, b)
            take("above", 0, *half, a)
        for j in range(own_rows - 1):
            for k in range(senders):
                take(j, k, lo, n, inner[c][j][k])
        meta = (tuple(pieces), rows_dev, cb, senders, own_rows)
        part, sums = pl.pallas_call(
            functools.partial(defect_kernel, meta, lo, n, group, amplitude),
            out_shape=(
                jax.ShapeDtypeStruct((n * per, LANES), jnp.float32),
                jax.ShapeDtypeStruct((group * peers if lo + n == group else group, LANES), jnp.float32),
            ),
            in_specs=[smem, vmem] + [vmem] * len(ins) + ([vmem] if lo else []),
            out_specs=(vmem, vmem),
            scratch_shapes=[
                pltpu.VMEM((rows_dev + 2, n * cb + PAD + TAIL, LANES), jnp.float32),
            ],
            cost_estimate=pl.CostEstimate(flops=20 * n * per * LANES, bytes_accessed=8 * n * per * LANES, transcendentals=0),
            compiler_params=pltpu.CompilerParams(vmem_limit_bytes=24 << 20),
            name="defect",
        )(source_index, weights, *ins, *([sums] if lo else []))
        parts.append(part)
    sums = lax.all_to_all(sums, "vtx", 0, 0, tiled=True)
    out, norms = pl.pallas_call(
        functools.partial(scale_kernel, chunks, float(total_rows * width)),
        out_shape=(
            jax.ShapeDtypeStruct((group * per, LANES), jnp.float32),
            jax.ShapeDtypeStruct((1, group), jnp.float32),
        ),
        in_specs=[vmem] + [vmem] * len(parts),
        out_specs=(pl.BlockSpec(memory_space=pltpu.HBM), vmem),
        scratch_shapes=[
            pltpu.VMEM((group * per + group, LANES), jnp.float32),
            pltpu.SemaphoreType.DMA((group,)),
        ],
        cost_estimate=pl.CostEstimate(flops=group * per * LANES, bytes_accessed=8 * group * per * LANES, transcendentals=0),
        compiler_params=pltpu.CompilerParams(vmem_limit_bytes=12 << 20),
        name="scale",
    )(sums, *parts)
    out = out.reshape(group, cb, rows_dev, LANES).transpose(0, 2, 1, 3).reshape(group, rows_dev, width)
    return out, norms.reshape(group)


def solution(mesh):
    return jax.shard_map(
        program,
        mesh=mesh,
        in_specs=(P(None, ("vtx", "src"), None), P(None, "vtx", None), P()),
        out_specs=(P("src", "vtx", None), P("src")),
        check_vma=False,
    )
```

```python
import functools
import math

import jax
import jax.numpy as jnp
from jax import lax
from jax.experimental import pallas as pl
from jax.experimental.pallas import tpu as pltpu
from jax.sharding import PartitionSpec as P


LANES = 128
SUB = 8
PAD = 8
TAIL = 16


def pack_kernel(meta, heat, *refs):
    blocks, group, cb, own_rows, senders = meta
    n_out = max(out for *_, targets in blocks for out, *_ in targets) + 1
    outs = refs[:n_out]
    wide, in_sem = refs[n_out:]
    me = lax.axis_index("src")
    low = me < senders // 2
    reads, at = [], 0
    for b, (k, lo, n, _) in enumerate(blocks):
        size = n * cb * own_rows
        copy = pltpu.make_async_copy(
            heat.at[pl.ds(((me ^ k) * group + lo) * cb * own_rows, size), :], wide.at[pl.ds(at, size), :], in_sem.at[b]
        )
        copy.start()
        reads.append((copy, at))
        at += size
    for (copy, at), (k, lo, n, targets) in zip(reads, blocks, strict=True):
        copy.wait()
        for out, rows, skip, first, count in targets:
            start = at + skip * cb * own_rows + jnp.where(low, rows[0], rows[1])

            def step(i, _, start=start, ref=outs[out], first=first):
                for u in range(cb // SUB):
                    to = pl.multiple_of((first + i) * cb + u * SUB, SUB)
                    ref[pl.ds(to, SUB), :] = wide[pl.ds(start + (i * cb + u * SUB) * own_rows, SUB, stride=own_rows), :]
                return 0

            lax.fori_loop(0, count, step, 0)


def pack(heat, wanted, blocks, group, cb, own_rows, senders, limit):
    plan = []
    for k, lo, n in blocks:
        targets = []
        for out, (wk, rows, first, count) in enumerate(wanted):
            begin, end = max(lo, first), min(lo + n, first + count)
            if wk == k and begin < end:
                targets.append((out, rows, begin - lo, begin - first, end - begin))
        plan.append((k, lo, n, tuple(targets)))
    reads = sum(n for _, n in ((k, n) for k, _, n in blocks)) * cb * own_rows
    writes = sum(count for *_, count in wanted) * cb
    vmem = pl.BlockSpec(memory_space=pltpu.VMEM)
    return pl.pallas_call(
        functools.partial(pack_kernel, (tuple(plan), group, cb, own_rows, senders)),
        out_shape=tuple(jax.ShapeDtypeStruct((count * cb, LANES), jnp.float32) for *_, count in wanted),
        in_specs=[pl.BlockSpec(memory_space=pltpu.HBM)],
        out_specs=tuple(vmem for _ in wanted),
        scratch_shapes=[
            pltpu.VMEM((reads, LANES), jnp.float32),
            pltpu.SemaphoreType.DMA((len(blocks),)),
        ],
        compiler_params=pltpu.CompilerParams(vmem_limit_bytes=limit << 20),
        cost_estimate=pl.CostEstimate(flops=writes * LANES, bytes_accessed=4 * (reads + writes) * LANES, transcendentals=0),
    )(heat)


def weights_kernel(meta, cotan, lower, out):
    rows_dev, cb, total_rows = meta
    block_start = lax.axis_index("vtx") * rows_dev
    lane = lax.broadcasted_iota(jnp.int32, (SUB, LANES), 1)
    index = lax.broadcasted_iota(jnp.int32, (SUB, LANES), 0) * LANES + lane
    last_lane = lane == LANES - 1

    def column_step(q, _):
        at = pl.ds(pl.multiple_of(q * SUB, SUB), SUB)
        inside_left = index + q * SUB * LANES > 0
        inside_right = index + q * SUB * LANES < cb * LANES - 1

        def row_of(array, row, back=0):
            return cotan[pl.ds((array * cb + q * SUB - back) * rows_dev + row, SUB, stride=rows_dev), :]

        def from_left(value, before):
            moved = pltpu.roll(jnp.where(last_lane, before, value), 1, 1)
            return jnp.where(inside_left, moved, 0.0)

        south = lower[pl.ds(pl.multiple_of(q * SUB, SUB), SUB), :]
        southwest = from_left(
            lower[pl.ds(pl.multiple_of(cb + q * SUB, SUB), SUB), :], lower[pl.ds(cb - 1 + q * SUB, SUB), :]
        )
        for row in range(rows_dev):
            inside_row = jnp.full((SUB, LANES), block_start + row, jnp.int32) < total_rows - 1
            east = row_of(1, row)
            west = from_left(east, row_of(1, row, 1))
            east = jnp.where(inside_right, east, 0.0)
            north = jnp.where(inside_row, row_of(2, row), 0.0)
            raw = row_of(3, row)
            diag = jnp.where(inside_right & inside_row, raw, 0.0)
            centre = row_of(0, row) + east + west + north + south + diag + southwest
            for w, value in enumerate((centre, east, west, north, south, diag, southwest)):
                out[w, row, at, :] = value
            south, southwest = north, from_left(raw, row_of(3, row, 1))
        return 0

    lax.fori_loop(0, cb // SUB, column_step, 0)


def defect_kernel(meta, lo, n, group, amplitude, *refs):
    pieces, rows_dev, cb, senders, own_rows = meta
    n_in = len(pieces)
    sources, weights = refs[:2]
    ins = refs[2 : 2 + n_in]
    prev = refs[2 + n_in] if lo else None
    out, sums, grid = refs[-3:]
    me = lax.axis_index("src")
    for ref, (kind, k, first, count, skip) in zip(ins, pieces, strict=True):
        t = me ^ k
        low = t < senders // 2
        if kind == "below":
            row = 0
        elif kind == "above":
            row = rows_dev + 1
        elif kind == "outer":
            row = 1 + t * own_rows + jnp.where(low, 0, own_rows - 1)
        else:
            row = 1 + t * own_rows + kind + jnp.where(low, 1, 0)

        def move(i, _, ref=ref, row=row, first=first, skip=skip):
            for u in range(cb // SUB):
                to = pl.multiple_of(PAD + (first - lo + i) * cb + u * SUB, SUB)
                grid[row, pl.ds(to, SUB), :] = ref[pl.ds(pl.multiple_of((skip + i) * cb + u * SUB, SUB), SUB), :]
            return 0

        lax.fori_loop(0, count, move, 0)
    zero = jnp.zeros((SUB, LANES), jnp.float32)
    for row in range(rows_dev + 2):
        grid[row, pl.ds(0, PAD), :] = zero
        grid[row, pl.ds(PAD + n * cb, PAD), :] = zero
    if lo:
        sums[pl.ds(0, group), :] = prev[...]
    else:
        sums[...] = jnp.zeros(sums.shape, jnp.float32)
    lane = lax.broadcasted_iota(jnp.int32, (SUB, LANES), 1)
    index = lax.broadcasted_iota(jnp.int32, (SUB, LANES), 0) * LANES + lane
    first_lane, last_lane = lane == 0, lane == LANES - 1
    width = cb * LANES
    start = lax.axis_index("vtx") * rows_dev * width

    def source_step(i, _):
        source = sources[me * group + lo + i] - start

        def column_step(q, total):
            base = pl.multiple_of(PAD + i * cb + q * SUB, SUB)
            at = pl.ds(pl.multiple_of(q * SUB, SUB), SUB)
            here, right, left = [], [], []
            for row in range(rows_dev + 2):
                value = grid[row, pl.ds(base, SUB), :]
                here.append(value)
                after = grid[row, pl.ds(base + 1, SUB), :] if row else None
                right.append(pltpu.roll(jnp.where(first_lane, after, value), LANES - 1, 1) if row else None)
                if row <= rows_dev:
                    before = grid[row, pl.ds(base - 1, SUB), :]
                    left.append(pltpu.roll(jnp.where(last_lane, before, value), 1, 1))
            for row in range(rows_dev):
                c = [weights[w, row, at, :] for w in range(7)]
                value = c[0] * here[row + 1] - c[1] * right[row + 1] - c[2] * left[row + 1]
                value = value - c[3] * here[row + 2] - c[4] * here[row]
                value = value - c[5] * right[row + 2] - c[6] * left[row]
                spot = source - row * width - q * SUB * LANES
                value = value - jnp.where(index == spot, amplitude, 0.0)
                out[pl.ds((i * cb + q * SUB) * rows_dev + row, SUB, stride=rows_dev), :] = value
                total = total + value * value
            return total

        total = lax.fori_loop(0, cb // SUB, column_step, zero, unroll=math.gcd(cb // SUB, 8))
        sums[pl.ds(lo + i, 1), :] = jnp.sum(total, axis=0, keepdims=True)
        return 0

    lax.fori_loop(0, n, source_step, 0)
    for first in range(group, sums.shape[0], group):
        sums[pl.ds(first, group), :] = sums[pl.ds(0, group), :]


def scale_kernel(chunks, size, *refs):
    total, parts, out, norms, buf, spread, out_sem = refs[0], refs[1:-5], *refs[-5:]
    group = sum(n for _, n in chunks)
    per = out.shape[0] // group
    sums = total[pl.ds(0, group), :]
    for first in range(group, total.shape[0], group):
        sums = sums + total[pl.ds(first, group), :]
    sums = jnp.sum(sums, axis=1, keepdims=True)
    norm = jnp.sqrt(sums / size + 1e-06)
    lane = lax.broadcasted_iota(jnp.int32, (group, LANES), 1)
    sub = lax.broadcasted_iota(jnp.int32, (group, LANES), 0)
    diagonal = jnp.where(lane == sub, jnp.broadcast_to(norm, (group, LANES)), 0.0)
    spread[...] = jnp.sum(diagonal, axis=0, keepdims=True)[:, :group]
    norms_copy = pltpu.make_async_copy(spread, norms, out_sem.at[group])
    norms_copy.start()
    buf[pl.ds(group * per, group), :] = jnp.broadcast_to(1.0 / norm, (group, LANES))

    def copy_of(i):
        spot = pl.ds(pl.multiple_of(i * per, per), per)
        return pltpu.make_async_copy(buf.at[spot, :], out.at[spot, :], out_sem.at[i])

    for part, (lo, n) in zip(parts, chunks, strict=True):

        def step(i, _, part=part, lo=lo):
            factor = jnp.broadcast_to(buf[pl.ds(group * per + lo + i, 1), :], (SUB, LANES))
            for at in range(0, per, SUB):
                to = pl.ds(pl.multiple_of((lo + i) * per + at, SUB), SUB)
                buf[to, :] = part[pl.ds(pl.multiple_of(i * per + at, SUB), SUB), :] * factor
            copy_of(lo + i).start()
            return 0

        lax.fori_loop(0, n, step, 0)

    def finish(i, _):
        copy_of(i).wait()
        return 0

    lax.fori_loop(0, group, finish, 0)
    norms_copy.wait()


def program(heat, cotan, source_index):
    peers, senders = lax.axis_size("vtx"), lax.axis_size("src")
    all_sources, own_rows, width = heat.shape
    rows_dev = cotan.shape[1]
    total_rows = rows_dev * peers
    group = all_sources // senders
    cb = width // LANES
    amplitude = math.sqrt(total_rows * width) / 8.0
    me = lax.axis_index("src")
    view = heat.reshape(all_sources, own_rows, cb, LANES).transpose(0, 2, 1, 3).reshape(-1, LANES)
    outer_rows = (0, own_rows - 1)
    order = [k for k in range(1, senders) if k >= 2] + [1]
    halves = [(0, group // 2), (group // 2, group - group // 2)]
    cuts = (0, group // 2, group - group * 3 // 16, group)
    chunks = [(lo, hi - lo) for lo, hi in zip(cuts[:-1], cuts[1:], strict=True) if hi > lo]
    common = (group, cb, own_rows, senders)

    def send(k, piece):
        return lax.ppermute(piece, "src", [(i, i ^ k) for i in range(senders)]) if k else piece

    wanted = [(k, outer_rows, *half) for half in halves for k in (1, 0)]
    wanted += [(k, (1 + j, j), *chunk) for chunk in chunks for j in range(own_rows - 1) for k in order + [0]]
    table = {}
    for half in halves:
        early = [(k, outer_rows, *half) for k in order[:-1]]
        packed = pack(view, early, [(k, *half) for k in order[:-1]], *common, 60)
        table.update(zip(early, packed, strict=True))
    packed = pack(view, wanted, [(k, *half) for half in halves for k in order + [0]], *common, 60)
    table.update(zip(wanted, packed, strict=True))
    for key, piece in table.items():
        table[key] = send(key[0], piece)
    outer = [{k: table[k, outer_rows, *half] for k in range(senders)} for half in halves]
    inner = [
        [{k: table[k, (1 + j, j), *chunk] for k in range(senders)} for j in range(own_rows - 1)] for chunk in chunks
    ]
    up = [(i, i + 1) for i in range(peers - 1)]
    down = [(j, i) for i, j in up]
    vmem = pl.BlockSpec(memory_space=pltpu.VMEM)
    smem = pl.BlockSpec(memory_space=pltpu.SMEM)
    per = cb * rows_dev
    lower = lax.ppermute(cotan[2:4, rows_dev - 1].reshape(2 * cb, LANES), "vtx", up)
    tiles = cotan.reshape(4, rows_dev, cb, LANES).transpose(0, 2, 1, 3).reshape(4 * per, LANES)
    weights = pl.pallas_call(
        functools.partial(weights_kernel, (rows_dev, cb, total_rows)),
        out_shape=jax.ShapeDtypeStruct((7, rows_dev, cb + PAD, LANES), jnp.float32),
        in_specs=[vmem, vmem],
        out_specs=vmem,
        compiler_params=pltpu.CompilerParams(vmem_limit_bytes=8 << 20),
        cost_estimate=pl.CostEstimate(flops=20 * per * LANES, bytes_accessed=44 * per * LANES, transcendentals=0),
        name="weights",
    )(tiles, lower)
    below, above = [], []
    for got in outer:
        first = lax.select_n(me, *[got[k] for k in range(senders)])
        last = lax.select_n(me, *[got[k] for k in reversed(range(senders))])
        above.append(lax.ppermute(first, "vtx", down))
        below.append(lax.ppermute(last, "vtx", up))

    parts, sums = [], None
    for c, (lo, n) in enumerate(chunks):
        pieces, ins = [], []

        def take(kind, k, first, count, array):
            begin, end = max(first, lo), min(first + count, lo + n)
            if begin < end:
                pieces.append((kind, k, begin, end - begin, begin - first))
                ins.append(array)

        for half, got, b, a in zip(halves, outer, below, above, strict=True):
            for k in range(senders):
                take("outer", k, *half, got[k])
            take("below", 0, *half, b)
            take("above", 0, *half, a)
        for j in range(own_rows - 1):
            for k in range(senders):
                take(j, k, lo, n, inner[c][j][k])
        meta = (tuple(pieces), rows_dev, cb, senders, own_rows)
        part, sums = pl.pallas_call(
            functools.partial(defect_kernel, meta, lo, n, group, amplitude),
            out_shape=(
                jax.ShapeDtypeStruct((n * per, LANES), jnp.float32),
                jax.ShapeDtypeStruct((group * peers if lo + n == group else group, LANES), jnp.float32),
            ),
            in_specs=[smem, vmem] + [vmem] * len(ins) + ([vmem] if lo else []),
            out_specs=(vmem, vmem),
            scratch_shapes=[
                pltpu.VMEM((rows_dev + 2, n * cb + PAD + TAIL, LANES), jnp.float32),
            ],
            cost_estimate=pl.CostEstimate(flops=20 * n * per * LANES, bytes_accessed=8 * n * per * LANES, transcendentals=0),
            compiler_params=pltpu.CompilerParams(vmem_limit_bytes=24 << 20),
            name="defect",
        )(source_index, weights, *ins, *([sums] if lo else []))
        parts.append(part)
    sums = lax.all_to_all(sums, "vtx", 0, 0, tiled=True)
    out, norms = pl.pallas_call(
        functools.partial(scale_kernel, chunks, float(total_rows * width)),
        out_shape=(
            jax.ShapeDtypeStruct((group * per, LANES), jnp.float32),
            jax.ShapeDtypeStruct((1, group), jnp.float32),
        ),
        in_specs=[vmem] + [vmem] * len(parts),
        out_specs=(pl.BlockSpec(memory_space=pltpu.HBM), pl.BlockSpec(memory_space=pltpu.HBM)),
        scratch_shapes=[
            pltpu.VMEM((group * per + group, LANES), jnp.float32),
            pltpu.VMEM((1, group), jnp.float32),
            pltpu.SemaphoreType.DMA((group + 1,)),
        ],
        cost_estimate=pl.CostEstimate(flops=group * per * LANES, bytes_accessed=8 * group * per * LANES, transcendentals=0),
        compiler_params=pltpu.CompilerParams(vmem_limit_bytes=12 << 20),
        name="scale",
    )(sums, *parts)
    out = out.reshape(group, cb, rows_dev, LANES).transpose(0, 2, 1, 3).reshape(group, rows_dev, width)
    return out, norms.reshape(group)


def solution(mesh):
    return jax.shard_map(
        program,
        mesh=mesh,
        in_specs=(P(None, ("vtx", "src"), None), P(None, "vtx", None), P()),
        out_specs=(P("src", "vtx", None), P("src")),
        check_vma=False,
    )
```

```python
import functools
import math

import jax
import jax.numpy as jnp
from jax import lax
from jax.experimental import pallas as pl
from jax.experimental.pallas import tpu as pltpu
from jax.sharding import PartitionSpec as P


LANES = 128
SUB = 8
PAD = 8
TAIL = 16


def pack_kernel(meta, heat, *refs):
    blocks, group, cb, own_rows, senders = meta
    n_out = max(out for *_, targets in blocks for out, *_ in targets) + 1
    outs = refs[:n_out]
    wide, in_sem = refs[n_out:]
    me = lax.axis_index("src")
    low = me < senders // 2
    reads, at = [], 0
    for b, (k, lo, n, _) in enumerate(blocks):
        size = n * cb * own_rows
        copy = pltpu.make_async_copy(
            heat.at[pl.ds(((me ^ k) * group + lo) * cb * own_rows, size), :], wide.at[pl.ds(at, size), :], in_sem.at[b]
        )
        copy.start()
        reads.append((copy, at))
        at += size
    for (copy, at), (k, lo, n, targets) in zip(reads, blocks, strict=True):
        copy.wait()
        for out, rows, skip, first, count in targets:
            start = at + skip * cb * own_rows + jnp.where(low, rows[0], rows[1])

            def step(i, _, start=start, ref=outs[out], first=first):
                for u in range(cb // SUB):
                    to = pl.multiple_of((first + i) * cb + u * SUB, SUB)
                    ref[pl.ds(to, SUB), :] = wide[pl.ds(start + (i * cb + u * SUB) * own_rows, SUB, stride=own_rows), :]
                return 0

            lax.fori_loop(0, count, step, 0)


def pack(heat, wanted, blocks, group, cb, own_rows, senders, limit):
    plan = []
    for k, lo, n in blocks:
        targets = []
        for out, (wk, rows, first, count) in enumerate(wanted):
            begin, end = max(lo, first), min(lo + n, first + count)
            if wk == k and begin < end:
                targets.append((out, rows, begin - lo, begin - first, end - begin))
        plan.append((k, lo, n, tuple(targets)))
    reads = sum(n for _, n in ((k, n) for k, _, n in blocks)) * cb * own_rows
    writes = sum(count for *_, count in wanted) * cb
    vmem = pl.BlockSpec(memory_space=pltpu.VMEM)
    return pl.pallas_call(
        functools.partial(pack_kernel, (tuple(plan), group, cb, own_rows, senders)),
        out_shape=tuple(jax.ShapeDtypeStruct((count * cb, LANES), jnp.float32) for *_, count in wanted),
        in_specs=[pl.BlockSpec(memory_space=pltpu.HBM)],
        out_specs=tuple(vmem for _ in wanted),
        scratch_shapes=[
            pltpu.VMEM((reads, LANES), jnp.float32),
            pltpu.SemaphoreType.DMA((len(blocks),)),
        ],
        compiler_params=pltpu.CompilerParams(vmem_limit_bytes=limit << 20),
        cost_estimate=pl.CostEstimate(flops=writes * LANES, bytes_accessed=4 * (reads + writes) * LANES, transcendentals=0),
    )(heat)


def weights_kernel(meta, sources, cotan, lower, out, spots):
    rows_dev, cb, total_rows = meta
    block_start = lax.axis_index("vtx") * rows_dev
    group = spots.shape[0]
    first = lax.axis_index("src") * group
    for i in range(group):
        spots[pl.ds(i, 1), :] = jnp.full((1, LANES), sources[first + i] - block_start * cb * LANES, jnp.int32)
    lane = lax.broadcasted_iota(jnp.int32, (SUB, LANES), 1)
    index = lax.broadcasted_iota(jnp.int32, (SUB, LANES), 0) * LANES + lane
    last_lane = lane == LANES - 1

    def column_step(q, _):
        at = pl.ds(pl.multiple_of(q * SUB, SUB), SUB)
        inside_left = index + q * SUB * LANES > 0
        inside_right = index + q * SUB * LANES < cb * LANES - 1

        def row_of(array, row, back=0):
            return cotan[pl.ds((array * cb + q * SUB - back) * rows_dev + row, SUB, stride=rows_dev), :]

        def from_left(value, before):
            moved = pltpu.roll(jnp.where(last_lane, before, value), 1, 1)
            return jnp.where(inside_left, moved, 0.0)

        south = lower[pl.ds(pl.multiple_of(q * SUB, SUB), SUB), :]
        southwest = from_left(
            lower[pl.ds(pl.multiple_of(cb + q * SUB, SUB), SUB), :], lower[pl.ds(cb - 1 + q * SUB, SUB), :]
        )
        for row in range(rows_dev):
            inside_row = jnp.full((SUB, LANES), block_start + row, jnp.int32) < total_rows - 1
            east = row_of(1, row)
            west = from_left(east, row_of(1, row, 1))
            east = jnp.where(inside_right, east, 0.0)
            north = jnp.where(inside_row, row_of(2, row), 0.0)
            raw = row_of(3, row)
            diag = jnp.where(inside_right & inside_row, raw, 0.0)
            centre = row_of(0, row) + east + west + north + south + diag + southwest
            for w, value in enumerate((centre, east, west, north, south, diag, southwest)):
                out[w, row, at, :] = value
            south, southwest = north, from_left(raw, row_of(3, row, 1))
        return 0

    lax.fori_loop(0, cb // SUB, column_step, 0)


def defect_kernel(meta, lo, n, group, amplitude, *refs):
    pieces, rows_dev, cb, senders, own_rows = meta
    n_in = len(pieces)
    spots, weights = refs[:2]
    ins = refs[2 : 2 + n_in]
    prev = refs[2 + n_in] if lo else None
    last = lo + n == group
    out, sums, grid = refs[-4:-1] if last else refs[-3:]
    total_of = refs[-1] if last else sums
    me = lax.axis_index("src")
    for ref, (kind, k, first, count, skip) in zip(ins, pieces, strict=True):
        t = me ^ k
        low = t < senders // 2
        if kind == "below":
            row = 0
        elif kind == "above":
            row = rows_dev + 1
        elif kind == "outer":
            row = 1 + t * own_rows + jnp.where(low, 0, own_rows - 1)
        else:
            row = 1 + t * own_rows + kind + jnp.where(low, 1, 0)

        def move(i, _, ref=ref, row=row, first=first, skip=skip):
            for u in range(cb // SUB):
                to = pl.multiple_of(PAD + (first - lo + i) * cb + u * SUB, SUB)
                grid[row, pl.ds(to, SUB), :] = ref[pl.ds(pl.multiple_of((skip + i) * cb + u * SUB, SUB), SUB), :]
            return 0

        lax.fori_loop(0, count, move, 0)
    zero = jnp.zeros((SUB, LANES), jnp.float32)
    for row in range(rows_dev + 2):
        grid[row, pl.ds(0, PAD), :] = zero
        grid[row, pl.ds(PAD + n * cb, PAD), :] = zero
    total_of[...] = prev[...] if lo else jnp.zeros((group, LANES), jnp.float32)
    lane = lax.broadcasted_iota(jnp.int32, (SUB, LANES), 1)
    index = lax.broadcasted_iota(jnp.int32, (SUB, LANES), 0) * LANES + lane
    first_lane, last_lane = lane == 0, lane == LANES - 1
    width = cb * LANES

    def source_step(i, _):
        spot = jnp.broadcast_to(spots[pl.ds(lo + i, 1), :], (SUB, LANES)) - index

        def column_step(q, total):
            base = pl.multiple_of(PAD + i * cb + q * SUB, SUB)
            at = pl.ds(pl.multiple_of(q * SUB, SUB), SUB)
            here, right, left = [], [], []
            for row in range(rows_dev + 2):
                value = grid[row, pl.ds(base, SUB), :]
                here.append(value)
                after = grid[row, pl.ds(base + 1, SUB), :] if row else None
                right.append(pltpu.roll(jnp.where(first_lane, after, value), LANES - 1, 1) if row else None)
                if row <= rows_dev:
                    before = grid[row, pl.ds(base - 1, SUB), :]
                    left.append(pltpu.roll(jnp.where(last_lane, before, value), 1, 1))
            for row in range(rows_dev):
                c = [weights[w, row, at, :] for w in range(7)]
                value = c[0] * here[row + 1] - c[1] * right[row + 1] - c[2] * left[row + 1]
                value = value - c[3] * here[row + 2] - c[4] * here[row]
                value = value - c[5] * right[row + 2] - c[6] * left[row]
                value = value - jnp.where(spot == row * width + q * SUB * LANES, amplitude, 0.0)
                out[pl.ds((i * cb + q * SUB) * rows_dev + row, SUB, stride=rows_dev), :] = value
                total = total + value * value
            return total

        total = lax.fori_loop(0, cb // SUB, column_step, zero, unroll=math.gcd(cb // SUB, 8))
        total_of[pl.ds(lo + i, 1), :] = jnp.sum(total, axis=0, keepdims=True)
        return 0

    lax.fori_loop(0, n, source_step, 0, unroll=math.gcd(n, 2))
    if last:
        whole = jnp.sum(total_of[...], axis=1, keepdims=True)
        lane = lax.broadcasted_iota(jnp.int32, (group, LANES), 1)
        diagonal = lane == lax.broadcasted_iota(jnp.int32, (group, LANES), 0)
        row = jnp.sum(jnp.where(diagonal, whole, 0.0), axis=0, keepdims=True)
        sums[...] = jnp.broadcast_to(row, sums.shape)


def scale_kernel(chunks, size, *refs):
    total, parts, out, norms, buf, spread, out_sem = refs[0], refs[1:-5], *refs[-5:]
    group = sum(n for _, n in chunks)
    per = out.shape[0] // group
    norm = jnp.sqrt(jnp.sum(total[...], axis=0, keepdims=True) / size + 1e-06)
    spread[...] = norm[:, :group]
    norms_copy = pltpu.make_async_copy(spread, norms, out_sem.at[group])
    norms_copy.start()
    lane = lax.broadcasted_iota(jnp.int32, (group, LANES), 1)
    diagonal = lane == lax.broadcasted_iota(jnp.int32, (group, LANES), 0)
    inverse = jnp.sum(jnp.where(diagonal, 1.0 / norm, 0.0), axis=1, keepdims=True)
    buf[pl.ds(group * per, group), :] = jnp.broadcast_to(inverse, (group, LANES))

    def copy_of(i):
        spot = pl.ds(pl.multiple_of(i * per, per), per)
        return pltpu.make_async_copy(buf.at[spot, :], out.at[spot, :], out_sem.at[i])

    for part, (lo, n) in zip(parts, chunks, strict=True):

        def step(i, _, part=part, lo=lo):
            factor = jnp.broadcast_to(buf[pl.ds(group * per + lo + i, 1), :], (SUB, LANES))
            for at in range(0, per, SUB):
                to = pl.ds(pl.multiple_of((lo + i) * per + at, SUB), SUB)
                buf[to, :] = part[pl.ds(pl.multiple_of(i * per + at, SUB), SUB), :] * factor
            copy_of(lo + i).start()
            return 0

        lax.fori_loop(0, n, step, 0)

    def finish(i, _):
        copy_of(i).wait()
        return 0

    lax.fori_loop(0, group, finish, 0)
    norms_copy.wait()


def program(heat, cotan, source_index):
    peers, senders = lax.axis_size("vtx"), lax.axis_size("src")
    all_sources, own_rows, width = heat.shape
    rows_dev = cotan.shape[1]
    total_rows = rows_dev * peers
    group = all_sources // senders
    cb = width // LANES
    amplitude = math.sqrt(total_rows * width) / 8.0
    me = lax.axis_index("src")
    view = heat.reshape(all_sources, own_rows, cb, LANES).transpose(0, 2, 1, 3).reshape(-1, LANES)
    outer_rows = (0, own_rows - 1)
    order = [k for k in range(1, senders) if k >= 2] + [1]
    halves = [(0, group // 2), (group // 2, group - group // 2)]
    cuts = (0, group // 2, group - group // 4, group - group // 8, group)
    chunks = [(lo, hi - lo) for lo, hi in zip(cuts[:-1], cuts[1:], strict=True) if hi > lo]
    common = (group, cb, own_rows, senders)

    def send(k, piece):
        return lax.ppermute(piece, "src", [(i, i ^ k) for i in range(senders)]) if k else piece

    wanted = [(k, outer_rows, *half) for half in halves for k in (1, 0)]
    wanted += [(k, (1 + j, j), *chunk) for chunk in chunks for j in range(own_rows - 1) for k in order + [0]]
    table = {}
    early = [(k, outer_rows, *half) for half in halves for k in order[:-1]]
    for part in (early[:1], early[1:]):
        packed = pack(view, part, [(k, *at) for k, _, *at in part], *common, 60)
        table.update(zip(part, packed, strict=True))
    packed = pack(view, wanted, [(k, *half) for half in halves for k in order + [0]], *common, 60)
    table.update(zip(wanted, packed, strict=True))
    for key, piece in table.items():
        table[key] = send(key[0], piece)
    outer = [{k: table[k, outer_rows, *half] for k in range(senders)} for half in halves]
    inner = [
        [{k: table[k, (1 + j, j), *chunk] for k in range(senders)} for j in range(own_rows - 1)] for chunk in chunks
    ]
    up = [(i, i + 1) for i in range(peers - 1)]
    down = [(j, i) for i, j in up]
    vmem = pl.BlockSpec(memory_space=pltpu.VMEM)
    per = cb * rows_dev
    lower = lax.ppermute(cotan[2:4, rows_dev - 1].reshape(2 * cb, LANES), "vtx", up)
    tiles = cotan.reshape(4, rows_dev, cb, LANES).transpose(0, 2, 1, 3).reshape(4 * per, LANES)
    weights, spots = pl.pallas_call(
        functools.partial(weights_kernel, (rows_dev, cb, total_rows)),
        out_shape=(
            jax.ShapeDtypeStruct((7, rows_dev, cb + PAD, LANES), jnp.float32),
            jax.ShapeDtypeStruct((group, LANES), jnp.int32),
        ),
        in_specs=[pl.BlockSpec(memory_space=pltpu.SMEM), vmem, vmem],
        out_specs=(vmem, vmem),
        compiler_params=pltpu.CompilerParams(vmem_limit_bytes=8 << 20),
        cost_estimate=pl.CostEstimate(flops=20 * per * LANES, bytes_accessed=44 * per * LANES, transcendentals=0),
        name="weights",
    )(source_index, tiles, lower)
    below, above = [], []
    for got in outer:
        first = lax.select_n(me, *[got[k] for k in range(senders)])
        last = lax.select_n(me, *[got[k] for k in reversed(range(senders))])
        above.append(lax.ppermute(first, "vtx", down))
        below.append(lax.ppermute(last, "vtx", up))

    parts, sums = [], None
    for c, (lo, n) in enumerate(chunks):
        pieces, ins = [], []

        def take(kind, k, first, count, array):
            begin, end = max(first, lo), min(first + count, lo + n)
            if begin < end:
                pieces.append((kind, k, begin, end - begin, begin - first))
                ins.append(array)

        for half, got, b, a in zip(halves, outer, below, above, strict=True):
            for k in range(senders):
                take("outer", k, *half, got[k])
            take("below", 0, *half, b)
            take("above", 0, *half, a)
        for j in range(own_rows - 1):
            for k in range(senders):
                take(j, k, lo, n, inner[c][j][k])
        meta = (tuple(pieces), rows_dev, cb, senders, own_rows)
        part, sums = pl.pallas_call(
            functools.partial(defect_kernel, meta, lo, n, group, amplitude),
            out_shape=(
                jax.ShapeDtypeStruct((n * per, LANES), jnp.float32),
                jax.ShapeDtypeStruct((peers if lo + n == group else group, LANES), jnp.float32),
            ),
            in_specs=[vmem, vmem] + [vmem] * len(ins) + ([vmem] if lo else []),
            out_specs=(vmem, vmem),
            scratch_shapes=[
                pltpu.VMEM((rows_dev + 2, n * cb + PAD + TAIL, LANES), jnp.float32),
            ]
            + ([pltpu.VMEM((group, LANES), jnp.float32)] if lo + n == group else []),
            cost_estimate=pl.CostEstimate(flops=20 * n * per * LANES, bytes_accessed=8 * n * per * LANES, transcendentals=0),
            compiler_params=pltpu.CompilerParams(vmem_limit_bytes=24 << 20),
            name="defect",
        )(spots, weights, *ins, *([sums] if lo else []))
        parts.append(part)
    sums = lax.all_to_all(sums, "vtx", 0, 0, tiled=True)
    out, norms = pl.pallas_call(
        functools.partial(scale_kernel, chunks, float(total_rows * width)),
        out_shape=(
            jax.ShapeDtypeStruct((group * per, LANES), jnp.float32),
            jax.ShapeDtypeStruct((1, group), jnp.float32),
        ),
        in_specs=[vmem] + [vmem] * len(parts),
        out_specs=(pl.BlockSpec(memory_space=pltpu.HBM), pl.BlockSpec(memory_space=pltpu.HBM)),
        scratch_shapes=[
            pltpu.VMEM((group * per + group, LANES), jnp.float32),
            pltpu.VMEM((1, group), jnp.float32),
            pltpu.SemaphoreType.DMA((group + 1,)),
        ],
        cost_estimate=pl.CostEstimate(flops=group * per * LANES, bytes_accessed=8 * group * per * LANES, transcendentals=0),
        compiler_params=pltpu.CompilerParams(vmem_limit_bytes=12 << 20),
        name="scale",
    )(sums, *parts)
    out = out.reshape(group, cb, rows_dev, LANES).transpose(0, 2, 1, 3).reshape(group, rows_dev, width)
    return out, norms.reshape(group)


def solution(mesh):
    return jax.shard_map(
        program,
        mesh=mesh,
        in_specs=(P(None, ("vtx", "src"), None), P(None, "vtx", None), P()),
        out_specs=(P("src", "vtx", None), P("src")),
        check_vma=False,
    )
```

```python
import functools
import math

import jax
import jax.numpy as jnp
from jax import lax
from jax.experimental import pallas as pl
from jax.experimental.pallas import tpu as pltpu
from jax.sharding import PartitionSpec as P


LANES = 128
SUB = 8
PAD = 8
TAIL = 16


def pack_kernel(meta, heat, *refs):
    blocks, group, cb, own_rows, senders = meta
    n_out = max(out for *_, targets in blocks for out, *_ in targets) + 1
    outs = refs[:n_out]
    wide, in_sem = refs[n_out:]
    me = lax.axis_index("src")
    low = me < senders // 2
    reads, at = [], 0
    for b, (k, lo, n, _) in enumerate(blocks):
        size = n * cb * own_rows
        copy = pltpu.make_async_copy(
            heat.at[pl.ds(((me ^ k) * group + lo) * cb * own_rows, size), :], wide.at[pl.ds(at, size), :], in_sem.at[b]
        )
        copy.start()
        reads.append((copy, at))
        at += size
    for (copy, at), (k, lo, n, targets) in zip(reads, blocks, strict=True):
        copy.wait()
        for out, rows, skip, first, count in targets:
            start = at + skip * cb * own_rows + jnp.where(low, rows[0], rows[1])

            def step(i, _, start=start, ref=outs[out], first=first):
                for u in range(cb // SUB):
                    to = pl.multiple_of((first + i) * cb + u * SUB, SUB)
                    ref[pl.ds(to, SUB), :] = wide[pl.ds(start + (i * cb + u * SUB) * own_rows, SUB, stride=own_rows), :]
                return 0

            lax.fori_loop(0, count, step, 0)


def pack(heat, wanted, blocks, group, cb, own_rows, senders, limit):
    plan = []
    for k, lo, n in blocks:
        targets = []
        for out, (wk, rows, first, count) in enumerate(wanted):
            begin, end = max(lo, first), min(lo + n, first + count)
            if wk == k and begin < end:
                targets.append((out, rows, begin - lo, begin - first, end - begin))
        plan.append((k, lo, n, tuple(targets)))
    reads = sum(n for _, n in ((k, n) for k, _, n in blocks)) * cb * own_rows
    writes = sum(count for *_, count in wanted) * cb
    vmem = pl.BlockSpec(memory_space=pltpu.VMEM)
    return pl.pallas_call(
        functools.partial(pack_kernel, (tuple(plan), group, cb, own_rows, senders)),
        out_shape=tuple(jax.ShapeDtypeStruct((count * cb, LANES), jnp.float32) for *_, count in wanted),
        in_specs=[pl.BlockSpec(memory_space=pltpu.HBM)],
        out_specs=tuple(vmem for _ in wanted),
        scratch_shapes=[
            pltpu.VMEM((reads, LANES), jnp.float32),
            pltpu.SemaphoreType.DMA((len(blocks),)),
        ],
        compiler_params=pltpu.CompilerParams(vmem_limit_bytes=limit << 20),
        cost_estimate=pl.CostEstimate(flops=writes * LANES, bytes_accessed=4 * (reads + writes) * LANES, transcendentals=0),
    )(heat)


def weights_kernel(meta, sources, cotan, lower, out, spots):
    rows_dev, cb, total_rows = meta
    block_start = lax.axis_index("vtx") * rows_dev
    group = spots.shape[0]
    first = lax.axis_index("src") * group
    for i in range(group):
        spots[pl.ds(i, 1), :] = jnp.full((1, LANES), sources[first + i] - block_start * cb * LANES, jnp.int32)
    lane = lax.broadcasted_iota(jnp.int32, (SUB, LANES), 1)
    index = lax.broadcasted_iota(jnp.int32, (SUB, LANES), 0) * LANES + lane
    last_lane = lane == LANES - 1

    def column_step(q, _):
        at = pl.ds(pl.multiple_of(q * SUB, SUB), SUB)
        inside_left = index + q * SUB * LANES > 0
        inside_right = index + q * SUB * LANES < cb * LANES - 1

        def row_of(array, row, back=0):
            return cotan[pl.ds((array * cb + q * SUB - back) * rows_dev + row, SUB, stride=rows_dev), :]

        def from_left(value, before):
            moved = pltpu.roll(jnp.where(last_lane, before, value), 1, 1)
            return jnp.where(inside_left, moved, 0.0)

        south = lower[pl.ds(pl.multiple_of(q * SUB, SUB), SUB), :]
        southwest = from_left(
            lower[pl.ds(pl.multiple_of(cb + q * SUB, SUB), SUB), :], lower[pl.ds(cb - 1 + q * SUB, SUB), :]
        )
        for row in range(rows_dev):
            inside_row = jnp.full((SUB, LANES), block_start + row, jnp.int32) < total_rows - 1
            east = row_of(1, row)
            west = from_left(east, row_of(1, row, 1))
            east = jnp.where(inside_right, east, 0.0)
            north = jnp.where(inside_row, row_of(2, row), 0.0)
            raw = row_of(3, row)
            diag = jnp.where(inside_right & inside_row, raw, 0.0)
            centre = row_of(0, row) + east + west + north + south + diag + southwest
            for w, value in enumerate((centre, east, west, north, south, diag, southwest)):
                out[w, row, at, :] = value
            south, southwest = north, from_left(raw, row_of(3, row, 1))
        return 0

    lax.fori_loop(0, cb // SUB, column_step, 0)


def defect_kernel(meta, lo, n, group, amplitude, *refs):
    pieces, rows_dev, cb, senders, own_rows = meta
    n_in = len(pieces)
    spots, weights = refs[:2]
    ins = refs[2 : 2 + n_in]
    prev = refs[2 + n_in] if lo else None
    last = lo + n == group
    out, sums, grid = refs[-4:-1] if last else refs[-3:]
    total_of = refs[-1] if last else sums
    me = lax.axis_index("src")
    for ref, (kind, k, first, count, skip) in zip(ins, pieces, strict=True):
        t = me ^ k
        low = t < senders // 2
        if kind == "below":
            row = 0
        elif kind == "above":
            row = rows_dev + 1
        elif kind == "outer":
            row = 1 + t * own_rows + jnp.where(low, 0, own_rows - 1)
        else:
            row = 1 + t * own_rows + kind + jnp.where(low, 1, 0)

        def move(i, _, ref=ref, row=row, first=first, skip=skip):
            for u in range(cb // SUB):
                to = pl.multiple_of(PAD + (first - lo + i) * cb + u * SUB, SUB)
                grid[row, pl.ds(to, SUB), :] = ref[pl.ds(pl.multiple_of((skip + i) * cb + u * SUB, SUB), SUB), :]
            return 0

        lax.fori_loop(0, count, move, 0)
    zero = jnp.zeros((SUB, LANES), jnp.float32)
    for row in range(rows_dev + 2):
        grid[row, pl.ds(0, PAD), :] = zero
        grid[row, pl.ds(PAD + n * cb, PAD), :] = zero
    total_of[...] = prev[...] if lo else jnp.zeros((group, LANES), jnp.float32)
    lane = lax.broadcasted_iota(jnp.int32, (SUB, LANES), 1)
    index = lax.broadcasted_iota(jnp.int32, (SUB, LANES), 0) * LANES + lane
    first_lane, last_lane = lane == 0, lane == LANES - 1
    width = cb * LANES

    def source_step(i, _):
        spot = jnp.broadcast_to(spots[pl.ds(lo + i, 1), :], (SUB, LANES)) - index

        def column_step(q, total):
            base = pl.multiple_of(PAD + i * cb + q * SUB, SUB)
            at = pl.ds(pl.multiple_of(q * SUB, SUB), SUB)
            here, right, left = [], [], []
            for row in range(rows_dev + 2):
                value = grid[row, pl.ds(base, SUB), :]
                here.append(value)
                after = grid[row, pl.ds(base + 1, SUB), :] if row else None
                right.append(pltpu.roll(jnp.where(first_lane, after, value), LANES - 1, 1) if row else None)
                if row <= rows_dev:
                    before = grid[row, pl.ds(base - 1, SUB), :]
                    left.append(pltpu.roll(jnp.where(last_lane, before, value), 1, 1))
            for row in range(rows_dev):
                c = [weights[w, row, at, :] for w in range(7)]
                value = c[0] * here[row + 1] - c[1] * right[row + 1] - c[2] * left[row + 1]
                value = value - c[3] * here[row + 2] - c[4] * here[row]
                value = value - c[5] * right[row + 2] - c[6] * left[row]
                value = value - jnp.where(spot == row * width + q * SUB * LANES, amplitude, 0.0)
                out[pl.ds((i * cb + q * SUB) * rows_dev + row, SUB, stride=rows_dev), :] = value
                total = total + value * value
            return total

        total = lax.fori_loop(0, cb // SUB, column_step, zero, unroll=math.gcd(cb // SUB, 8))
        total_of[pl.ds(lo + i, 1), :] = jnp.sum(total, axis=0, keepdims=True)
        return 0

    lax.fori_loop(0, n, source_step, 0, unroll=math.gcd(n, 2))
    if last:
        whole = jnp.sum(total_of[...], axis=1, keepdims=True)
        lane = lax.broadcasted_iota(jnp.int32, (group, LANES), 1)
        diagonal = lane == lax.broadcasted_iota(jnp.int32, (group, LANES), 0)
        row = jnp.sum(jnp.where(diagonal, whole, 0.0), axis=0, keepdims=True)
        top = lax.broadcasted_iota(jnp.int32, sums.shape, 0) == 0
        sums[...] = jnp.where(top, row, 0.0)


def scale_kernel(chunks, size, *refs):
    total, other, parts, out, norms, buf, spread, out_sem = refs[0], refs[1], refs[2:-5], *refs[-5:]
    group = sum(n for _, n in chunks)
    per = out.shape[0] // group
    norm = jnp.sqrt(jnp.sum(total[...] + other[...], axis=0, keepdims=True) / size + 1e-06)
    spread[...] = norm[:, :group]
    norms_copy = pltpu.make_async_copy(spread, norms, out_sem.at[group])
    norms_copy.start()
    lane = lax.broadcasted_iota(jnp.int32, (group, LANES), 1)
    diagonal = lane == lax.broadcasted_iota(jnp.int32, (group, LANES), 0)
    inverse = jnp.sum(jnp.where(diagonal, 1.0 / norm, 0.0), axis=1, keepdims=True)
    buf[pl.ds(group * per, group), :] = jnp.broadcast_to(inverse, (group, LANES))

    def copy_of(i):
        spot = pl.ds(pl.multiple_of(i * per, per), per)
        return pltpu.make_async_copy(buf.at[spot, :], out.at[spot, :], out_sem.at[i])

    for part, (lo, n) in zip(parts, chunks, strict=True):

        def step(i, _, part=part, lo=lo):
            factor = jnp.broadcast_to(buf[pl.ds(group * per + lo + i, 1), :], (SUB, LANES))
            for at in range(0, per, SUB):
                to = pl.ds(pl.multiple_of((lo + i) * per + at, SUB), SUB)
                buf[to, :] = part[pl.ds(pl.multiple_of(i * per + at, SUB), SUB), :] * factor
            copy_of(lo + i).start()
            return 0

        lax.fori_loop(0, n, step, 0)

    def finish(i, _):
        copy_of(i).wait()
        return 0

    lax.fori_loop(0, group, finish, 0)
    norms_copy.wait()


def program(heat, cotan, source_index):
    peers, senders = lax.axis_size("vtx"), lax.axis_size("src")
    all_sources, own_rows, width = heat.shape
    rows_dev = cotan.shape[1]
    total_rows = rows_dev * peers
    group = all_sources // senders
    cb = width // LANES
    amplitude = math.sqrt(total_rows * width) / 8.0
    me = lax.axis_index("src")
    view = heat.reshape(all_sources, own_rows, cb, LANES).transpose(0, 2, 1, 3).reshape(-1, LANES)
    outer_rows = (0, own_rows - 1)
    order = [k for k in range(1, senders) if k >= 2] + [1]
    halves = [(0, group // 2), (group // 2, group - group // 2)]
    cuts = (0, group // 2, group - group // 4, group - group // 8, group)
    chunks = [(lo, hi - lo) for lo, hi in zip(cuts[:-1], cuts[1:], strict=True) if hi > lo]
    common = (group, cb, own_rows, senders)

    def send(k, piece):
        return lax.ppermute(piece, "src", [(i, i ^ k) for i in range(senders)]) if k else piece

    wanted = [(k, outer_rows, *half) for half in halves for k in (1, 0)]
    wanted += [(k, (1 + j, j), *chunk) for chunk in chunks for j in range(own_rows - 1) for k in order + [0]]
    table = {}
    early = [(k, outer_rows, *half) for half in halves for k in order[:-1]]
    for part in (early[:1], early[1:]):
        packed = pack(view, part, [(k, *at) for k, _, *at in part], *common, 60)
        table.update(zip(part, packed, strict=True))
    packed = pack(view, wanted, [(k, *half) for half in halves for k in order + [0]], *common, 60)
    table.update(zip(wanted, packed, strict=True))
    for key, piece in table.items():
        table[key] = send(key[0], piece)
    outer = [{k: table[k, outer_rows, *half] for k in range(senders)} for half in halves]
    inner = [
        [{k: table[k, (1 + j, j), *chunk] for k in range(senders)} for j in range(own_rows - 1)] for chunk in chunks
    ]
    up = [(i, i + 1) for i in range(peers - 1)]
    down = [(j, i) for i, j in up]
    vmem = pl.BlockSpec(memory_space=pltpu.VMEM)
    per = cb * rows_dev
    lower = lax.ppermute(cotan[2:4, rows_dev - 1].reshape(2 * cb, LANES), "vtx", up)
    tiles = cotan.reshape(4, rows_dev, cb, LANES).transpose(0, 2, 1, 3).reshape(4 * per, LANES)
    weights, spots = pl.pallas_call(
        functools.partial(weights_kernel, (rows_dev, cb, total_rows)),
        out_shape=(
            jax.ShapeDtypeStruct((7, rows_dev, cb + PAD, LANES), jnp.float32),
            jax.ShapeDtypeStruct((group, LANES), jnp.int32),
        ),
        in_specs=[pl.BlockSpec(memory_space=pltpu.SMEM), vmem, vmem],
        out_specs=(vmem, vmem),
        compiler_params=pltpu.CompilerParams(vmem_limit_bytes=8 << 20),
        cost_estimate=pl.CostEstimate(flops=20 * per * LANES, bytes_accessed=44 * per * LANES, transcendentals=0),
        name="weights",
    )(source_index, tiles, lower)
    below, above = [], []
    for got in outer:
        first = lax.select_n(me, *[got[k] for k in range(senders)])
        last = lax.select_n(me, *[got[k] for k in reversed(range(senders))])
        above.append(lax.ppermute(first, "vtx", down))
        below.append(lax.ppermute(last, "vtx", up))

    parts, sums = [], None
    for c, (lo, n) in enumerate(chunks):
        pieces, ins = [], []

        def take(kind, k, first, count, array):
            begin, end = max(first, lo), min(first + count, lo + n)
            if begin < end:
                pieces.append((kind, k, begin, end - begin, begin - first))
                ins.append(array)

        for half, got, b, a in zip(halves, outer, below, above, strict=True):
            for k in range(senders):
                take("outer", k, *half, got[k])
            take("below", 0, *half, b)
            take("above", 0, *half, a)
        for j in range(own_rows - 1):
            for k in range(senders):
                take(j, k, lo, n, inner[c][j][k])
        meta = (tuple(pieces), rows_dev, cb, senders, own_rows)
        part, sums = pl.pallas_call(
            functools.partial(defect_kernel, meta, lo, n, group, amplitude),
            out_shape=(
                jax.ShapeDtypeStruct((n * per, LANES), jnp.float32),
                jax.ShapeDtypeStruct((peers if lo + n == group else group, LANES), jnp.float32),
            ),
            in_specs=[vmem, vmem] + [vmem] * len(ins) + ([vmem] if lo else []),
            out_specs=(vmem, vmem),
            scratch_shapes=[
                pltpu.VMEM((rows_dev + 2, n * cb + PAD + TAIL, LANES), jnp.float32),
            ]
            + ([pltpu.VMEM((group, LANES), jnp.float32)] if lo + n == group else []),
            cost_estimate=pl.CostEstimate(flops=20 * n * per * LANES, bytes_accessed=8 * n * per * LANES, transcendentals=0),
            compiler_params=pltpu.CompilerParams(vmem_limit_bytes=24 << 20),
            name="defect",
        )(spots, weights, *ins, *([sums] if lo else []))
        parts.append(part)
    steps = [1 << i for i in range((peers - 1).bit_length())]
    for step in steps:
        other = lax.ppermute(sums, "vtx", [(i, i ^ step) for i in range(peers)])
        if step != steps[-1]:
            sums = sums + other
    out, norms = pl.pallas_call(
        functools.partial(scale_kernel, chunks, float(total_rows * width)),
        out_shape=(
            jax.ShapeDtypeStruct((group * per, LANES), jnp.float32),
            jax.ShapeDtypeStruct((1, group), jnp.float32),
        ),
        in_specs=[vmem, vmem] + [vmem] * len(parts),
        out_specs=(pl.BlockSpec(memory_space=pltpu.HBM), pl.BlockSpec(memory_space=pltpu.HBM)),
        scratch_shapes=[
            pltpu.VMEM((group * per + group, LANES), jnp.float32),
            pltpu.VMEM((1, group), jnp.float32),
            pltpu.SemaphoreType.DMA((group + 1,)),
        ],
        cost_estimate=pl.CostEstimate(flops=group * per * LANES, bytes_accessed=8 * group * per * LANES, transcendentals=0),
        compiler_params=pltpu.CompilerParams(vmem_limit_bytes=12 << 20),
        name="scale",
    )(sums, other, *parts)
    out = out.reshape(group, cb, rows_dev, LANES).transpose(0, 2, 1, 3).reshape(group, rows_dev, width)
    return out, norms.reshape(group)


def solution(mesh):
    return jax.shard_map(
        program,
        mesh=mesh,
        in_specs=(P(None, ("vtx", "src"), None), P(None, "vtx", None), P()),
        out_specs=(P("src", "vtx", None), P("src")),
        check_vma=False,
    )
```

```python
import functools
import math

import jax
import jax.numpy as jnp
from jax import lax
from jax.experimental import pallas as pl
from jax.experimental.pallas import tpu as pltpu
from jax.sharding import PartitionSpec as P


LANES = 128
SUB = 8
PAD = 8
TAIL = 16


def pack_kernel(meta, heat, *refs):
    blocks, group, cb, own_rows, senders = meta
    n_out = max(out for *_, targets in blocks for out, *_ in targets) + 1
    outs = refs[:n_out]
    wide, in_sem = refs[n_out:]
    me = lax.axis_index("src")
    low = me < senders // 2
    reads, at = [], 0
    for b, (k, lo, n, _) in enumerate(blocks):
        size = n * cb * own_rows
        copy = pltpu.make_async_copy(
            heat.at[pl.ds(((me ^ k) * group + lo) * cb * own_rows, size), :], wide.at[pl.ds(at, size), :], in_sem.at[b]
        )
        copy.start()
        reads.append((copy, at))
        at += size
    for (copy, at), (k, lo, n, targets) in zip(reads, blocks, strict=True):
        copy.wait()
        for out, rows, skip, first, count in targets:
            start = at + skip * cb * own_rows + jnp.where(low, rows[0], rows[1])

            def step(i, _, start=start, ref=outs[out], first=first):
                for u in range(cb // SUB):
                    to = pl.multiple_of((first + i) * cb + u * SUB, SUB)
                    ref[pl.ds(to, SUB), :] = wide[pl.ds(start + (i * cb + u * SUB) * own_rows, SUB, stride=own_rows), :]
                return 0

            lax.fori_loop(0, count, step, 0)


def pack(heat, wanted, blocks, group, cb, own_rows, senders, limit):
    plan = []
    for k, lo, n in blocks:
        targets = []
        for out, (wk, rows, first, count) in enumerate(wanted):
            begin, end = max(lo, first), min(lo + n, first + count)
            if wk == k and begin < end:
                targets.append((out, rows, begin - lo, begin - first, end - begin))
        plan.append((k, lo, n, tuple(targets)))
    reads = sum(n for _, n in ((k, n) for k, _, n in blocks)) * cb * own_rows
    writes = sum(count for *_, count in wanted) * cb
    vmem = pl.BlockSpec(memory_space=pltpu.VMEM)
    return pl.pallas_call(
        functools.partial(pack_kernel, (tuple(plan), group, cb, own_rows, senders)),
        out_shape=tuple(jax.ShapeDtypeStruct((count * cb, LANES), jnp.float32) for *_, count in wanted),
        in_specs=[pl.BlockSpec(memory_space=pltpu.HBM)],
        out_specs=tuple(vmem for _ in wanted),
        scratch_shapes=[
            pltpu.VMEM((reads, LANES), jnp.float32),
            pltpu.SemaphoreType.DMA((len(blocks),)),
        ],
        compiler_params=pltpu.CompilerParams(vmem_limit_bytes=limit << 20),
        cost_estimate=pl.CostEstimate(flops=writes * LANES, bytes_accessed=4 * (reads + writes) * LANES, transcendentals=0),
    )(heat)


def weights_kernel(meta, sources, cotan, lower, out, spots):
    rows_dev, cb, total_rows = meta
    block_start = lax.axis_index("vtx") * rows_dev
    group = spots.shape[0]
    first = lax.axis_index("src") * group
    for i in range(group):
        spots[pl.ds(i, 1), :] = jnp.full((1, LANES), sources[first + i] - block_start * cb * LANES, jnp.int32)
    lane = lax.broadcasted_iota(jnp.int32, (SUB, LANES), 1)
    index = lax.broadcasted_iota(jnp.int32, (SUB, LANES), 0) * LANES + lane
    last_lane = lane == LANES - 1

    def column_step(q, _):
        at = pl.ds(pl.multiple_of(q * SUB, SUB), SUB)
        inside_left = index + q * SUB * LANES > 0
        inside_right = index + q * SUB * LANES < cb * LANES - 1

        def row_of(array, row, back=0):
            return cotan[pl.ds((array * cb + q * SUB - back) * rows_dev + row, SUB, stride=rows_dev), :]

        def from_left(value, before):
            moved = pltpu.roll(jnp.where(last_lane, before, value), 1, 1)
            return jnp.where(inside_left, moved, 0.0)

        south = lower[pl.ds(pl.multiple_of(q * SUB, SUB), SUB), :]
        southwest = from_left(
            lower[pl.ds(pl.multiple_of(cb + q * SUB, SUB), SUB), :], lower[pl.ds(cb - 1 + q * SUB, SUB), :]
        )
        for row in range(rows_dev):
            inside_row = jnp.full((SUB, LANES), block_start + row, jnp.int32) < total_rows - 1
            east = row_of(1, row)
            west = from_left(east, row_of(1, row, 1))
            east = jnp.where(inside_right, east, 0.0)
            north = jnp.where(inside_row, row_of(2, row), 0.0)
            raw = row_of(3, row)
            diag = jnp.where(inside_right & inside_row, raw, 0.0)
            centre = row_of(0, row) + east + west + north + south + diag + southwest
            for w, value in enumerate((centre, east, west, north, south, diag, southwest)):
                out[w, row, at, :] = value
            south, southwest = north, from_left(raw, row_of(3, row, 1))
        return 0

    lax.fori_loop(0, cb // SUB, column_step, 0)


def defect_kernel(meta, lo, n, group, amplitude, *refs):
    pieces, rows_dev, cb, senders, own_rows = meta
    n_in = len(pieces)
    spots, weights = refs[:2]
    ins = refs[2 : 2 + n_in]
    prev = refs[2 + n_in] if lo else None
    last = lo + n == group
    out, sums, grid = refs[-4:-1] if last else refs[-3:]
    total_of = refs[-1] if last else sums
    me = lax.axis_index("src")
    for ref, (kind, k, first, count, skip) in zip(ins, pieces, strict=True):
        t = me ^ k
        low = t < senders // 2
        if kind == "below":
            row = 0
        elif kind == "above":
            row = rows_dev + 1
        elif kind == "outer":
            row = 1 + t * own_rows + jnp.where(low, 0, own_rows - 1)
        else:
            row = 1 + t * own_rows + kind + jnp.where(low, 1, 0)

        def move(i, _, ref=ref, row=row, first=first, skip=skip):
            for u in range(cb // SUB):
                to = pl.multiple_of(PAD + (first - lo + i) * cb + u * SUB, SUB)
                grid[row, pl.ds(to, SUB), :] = ref[pl.ds(pl.multiple_of((skip + i) * cb + u * SUB, SUB), SUB), :]
            return 0

        lax.fori_loop(0, count, move, 0)
    zero = jnp.zeros((SUB, LANES), jnp.float32)
    for row in range(rows_dev + 2):
        grid[row, pl.ds(0, PAD), :] = zero
        grid[row, pl.ds(PAD + n * cb, PAD), :] = zero
    total_of[...] = prev[...] if lo else jnp.zeros((group, LANES), jnp.float32)
    lane = lax.broadcasted_iota(jnp.int32, (SUB, LANES), 1)
    index = lax.broadcasted_iota(jnp.int32, (SUB, LANES), 0) * LANES + lane
    first_lane, last_lane = lane == 0, lane == LANES - 1
    width = cb * LANES

    def source_step(i, _):
        spot = jnp.broadcast_to(spots[pl.ds(lo + i, 1), :], (SUB, LANES)) - index

        def column_step(q, total):
            base = pl.multiple_of(PAD + i * cb + q * SUB, SUB)
            at = pl.ds(pl.multiple_of(q * SUB, SUB), SUB)
            here, right, left = [], [], []
            for row in range(rows_dev + 2):
                value = grid[row, pl.ds(base, SUB), :]
                here.append(value)
                after = grid[row, pl.ds(base + 1, SUB), :] if row else None
                right.append(pltpu.roll(jnp.where(first_lane, after, value), LANES - 1, 1) if row else None)
                if row <= rows_dev:
                    before = grid[row, pl.ds(base - 1, SUB), :]
                    left.append(pltpu.roll(jnp.where(last_lane, before, value), 1, 1))
            for row in range(rows_dev):
                c = [weights[w, row, at, :] for w in range(7)]
                value = c[0] * here[row + 1] - c[1] * right[row + 1] - c[2] * left[row + 1]
                value = value - c[3] * here[row + 2] - c[4] * here[row]
                value = value - c[5] * right[row + 2] - c[6] * left[row]
                value = value - jnp.where(spot == row * width + q * SUB * LANES, amplitude, 0.0)
                out[pl.ds((i * cb + q * SUB) * rows_dev + row, SUB, stride=rows_dev), :] = value
                total = total + value * value
            return total

        total = lax.fori_loop(0, cb // SUB, column_step, zero, unroll=math.gcd(cb // SUB, 8))
        total_of[pl.ds(lo + i, 1), :] = jnp.sum(total, axis=0, keepdims=True)
        return 0

    lax.fori_loop(0, n, source_step, 0, unroll=max(u for u in (1, 2, 3, 4) if n % u == 0))
    if last:
        whole = jnp.sum(total_of[...], axis=1, keepdims=True)
        lane = lax.broadcasted_iota(jnp.int32, (group, LANES), 1)
        diagonal = lane == lax.broadcasted_iota(jnp.int32, (group, LANES), 0)
        row = jnp.sum(jnp.where(diagonal, whole, 0.0), axis=0, keepdims=True)
        top = lax.broadcasted_iota(jnp.int32, sums.shape, 0) == 0
        sums[...] = jnp.where(top, row, 0.0)


def scale_kernel(chunks, size, *refs):
    total, other, parts, out, norms, buf, spread, out_sem = refs[0], refs[1], refs[2:-5], *refs[-5:]
    group = sum(n for _, n in chunks)
    per = out.shape[0] // group
    norm = jnp.sqrt(jnp.sum(total[...] + other[...], axis=0, keepdims=True) / size + 1e-06)
    spread[...] = norm[:, :group]
    norms_copy = pltpu.make_async_copy(spread, norms, out_sem.at[group])
    norms_copy.start()
    lane = lax.broadcasted_iota(jnp.int32, (group, LANES), 1)
    diagonal = lane == lax.broadcasted_iota(jnp.int32, (group, LANES), 0)
    inverse = jnp.sum(jnp.where(diagonal, 1.0 / norm, 0.0), axis=1, keepdims=True)
    buf[pl.ds(group * per, group), :] = jnp.broadcast_to(inverse, (group, LANES))

    def copy_of(i):
        spot = pl.ds(pl.multiple_of(i * per, per), per)
        return pltpu.make_async_copy(buf.at[spot, :], out.at[spot, :], out_sem.at[i])

    for part, (lo, n) in zip(parts, chunks, strict=True):

        def step(i, _, part=part, lo=lo):
            factor = jnp.broadcast_to(buf[pl.ds(group * per + lo + i, 1), :], (SUB, LANES))
            for at in range(0, per, SUB):
                to = pl.ds(pl.multiple_of((lo + i) * per + at, SUB), SUB)
                buf[to, :] = part[pl.ds(pl.multiple_of(i * per + at, SUB), SUB), :] * factor
            copy_of(lo + i).start()
            return 0

        lax.fori_loop(0, n, step, 0)

    def finish(i, _):
        copy_of(i).wait()
        return 0

    lax.fori_loop(0, group, finish, 0)
    norms_copy.wait()


def program(heat, cotan, source_index):
    peers, senders = lax.axis_size("vtx"), lax.axis_size("src")
    all_sources, own_rows, width = heat.shape
    rows_dev = cotan.shape[1]
    total_rows = rows_dev * peers
    group = all_sources // senders
    cb = width // LANES
    amplitude = math.sqrt(total_rows * width) / 8.0
    me = lax.axis_index("src")
    view = heat.reshape(all_sources, own_rows, cb, LANES).transpose(0, 2, 1, 3).reshape(-1, LANES)
    outer_rows = (0, own_rows - 1)
    order = [k for k in range(1, senders) if k >= 2] + [1]
    halves = [(0, group // 2), (group // 2, group - group // 2)]
    cuts = (0, group // 2, group - group // 8, group)
    chunks = [(lo, hi - lo) for lo, hi in zip(cuts[:-1], cuts[1:], strict=True) if hi > lo]
    common = (group, cb, own_rows, senders)

    def send(k, piece):
        return lax.ppermute(piece, "src", [(i, i ^ k) for i in range(senders)]) if k else piece

    wanted = [(k, outer_rows, *half) for half in halves for k in (1, 0)]
    wanted += [(k, (1 + j, j), *chunk) for chunk in chunks for j in range(own_rows - 1) for k in order + [0]]
    table = {}
    early = [(k, outer_rows, *half) for half in halves for k in order[:-1]]
    for part in (early[:1], early[1:]):
        packed = pack(view, part, [(k, *at) for k, _, *at in part], *common, 60)
        table.update(zip(part, packed, strict=True))
    packed = pack(view, wanted, [(k, *half) for half in halves for k in order + [0]], *common, 60)
    table.update(zip(wanted, packed, strict=True))
    for key, piece in table.items():
        table[key] = send(key[0], piece)
    outer = [{k: table[k, outer_rows, *half] for k in range(senders)} for half in halves]
    inner = [
        [{k: table[k, (1 + j, j), *chunk] for k in range(senders)} for j in range(own_rows - 1)] for chunk in chunks
    ]
    up = [(i, i + 1) for i in range(peers - 1)]
    down = [(j, i) for i, j in up]
    vmem = pl.BlockSpec(memory_space=pltpu.VMEM)
    per = cb * rows_dev
    lower = lax.ppermute(cotan[2:4, rows_dev - 1].reshape(2 * cb, LANES), "vtx", up)
    tiles = cotan.reshape(4, rows_dev, cb, LANES).transpose(0, 2, 1, 3).reshape(4 * per, LANES)
    weights, spots = pl.pallas_call(
        functools.partial(weights_kernel, (rows_dev, cb, total_rows)),
        out_shape=(
            jax.ShapeDtypeStruct((7, rows_dev, cb + PAD, LANES), jnp.float32),
            jax.ShapeDtypeStruct((group, LANES), jnp.int32),
        ),
        in_specs=[pl.BlockSpec(memory_space=pltpu.SMEM), vmem, vmem],
        out_specs=(vmem, vmem),
        compiler_params=pltpu.CompilerParams(vmem_limit_bytes=8 << 20),
        cost_estimate=pl.CostEstimate(flops=20 * per * LANES, bytes_accessed=44 * per * LANES, transcendentals=0),
        name="weights",
    )(source_index, tiles, lower)
    below, above = [], []
    for got in outer:
        first = lax.select_n(me, *[got[k] for k in range(senders)])
        last = lax.select_n(me, *[got[k] for k in reversed(range(senders))])
        above.append(lax.ppermute(first, "vtx", down))
        below.append(lax.ppermute(last, "vtx", up))

    parts, sums = [], None
    for c, (lo, n) in enumerate(chunks):
        pieces, ins = [], []

        def take(kind, k, first, count, array):
            begin, end = max(first, lo), min(first + count, lo + n)
            if begin < end:
                pieces.append((kind, k, begin, end - begin, begin - first))
                ins.append(array)

        for half, got, b, a in zip(halves, outer, below, above, strict=True):
            for k in range(senders):
                take("outer", k, *half, got[k])
            take("below", 0, *half, b)
            take("above", 0, *half, a)
        for j in range(own_rows - 1):
            for k in range(senders):
                take(j, k, lo, n, inner[c][j][k])
        meta = (tuple(pieces), rows_dev, cb, senders, own_rows)
        part, sums = pl.pallas_call(
            functools.partial(defect_kernel, meta, lo, n, group, amplitude),
            out_shape=(
                jax.ShapeDtypeStruct((n * per, LANES), jnp.float32),
                jax.ShapeDtypeStruct((SUB if lo + n == group else group, LANES), jnp.float32),
            ),
            in_specs=[vmem, vmem] + [vmem] * len(ins) + ([vmem] if lo else []),
            out_specs=(vmem, vmem),
            scratch_shapes=[
                pltpu.VMEM((rows_dev + 2, n * cb + PAD + TAIL, LANES), jnp.float32),
            ]
            + ([pltpu.VMEM((group, LANES), jnp.float32)] if lo + n == group else []),
            cost_estimate=pl.CostEstimate(flops=20 * n * per * LANES, bytes_accessed=8 * n * per * LANES, transcendentals=0),
            compiler_params=pltpu.CompilerParams(vmem_limit_bytes=24 << 20),
            name="defect",
        )(spots, weights, *ins, *([sums] if lo else []))
        parts.append(part)
    steps = [1 << i for i in range((peers - 1).bit_length())]
    for step in steps:
        other = lax.ppermute(sums, "vtx", [(i, i ^ step) for i in range(peers)])
        if step != steps[-1]:
            sums = sums + other
    out, norms = pl.pallas_call(
        functools.partial(scale_kernel, chunks, float(total_rows * width)),
        out_shape=(
            jax.ShapeDtypeStruct((group * per, LANES), jnp.float32),
            jax.ShapeDtypeStruct((1, group), jnp.float32),
        ),
        in_specs=[vmem, vmem] + [vmem] * len(parts),
        out_specs=(pl.BlockSpec(memory_space=pltpu.HBM), pl.BlockSpec(memory_space=pltpu.HBM)),
        scratch_shapes=[
            pltpu.VMEM((group * per + group, LANES), jnp.float32),
            pltpu.VMEM((1, group), jnp.float32),
            pltpu.SemaphoreType.DMA((group + 1,)),
        ],
        cost_estimate=pl.CostEstimate(flops=group * per * LANES, bytes_accessed=8 * group * per * LANES, transcendentals=0),
        compiler_params=pltpu.CompilerParams(vmem_limit_bytes=12 << 20),
        name="scale",
    )(sums, other, *parts)
    out = out.reshape(group, cb, rows_dev, LANES).transpose(0, 2, 1, 3).reshape(group, rows_dev, width)
    return out, norms.reshape(group)


def solution(mesh):
    return jax.shard_map(
        program,
        mesh=mesh,
        in_specs=(P(None, ("vtx", "src"), None), P(None, "vtx", None), P()),
        out_specs=(P("src", "vtx", None), P("src")),
        check_vma=False,
    )
```
